64 devices in a mesh: data: 4 (over x, y), stage: 16 (over z, core).
Axes of the slice: x: 2, y: 2, z: 8, core: 2. Of those that a mesh axis runs over, the one named last changes fastest.
The devices are a block of a 4x4x8 slice.
Arguments:
- inputs: bfloat16 [1024, 16, 512], P('data'), parts along dimension 0
- targets: bfloat16 [1024, 16, 512], P('data'), parts along dimension 0
- lengths: int32 [1024], P('data'), parts along dimension 0
- w_in: bfloat16 [16, 512, 2048], P('stage')
- w_rec: bfloat16 [16, 512, 2048], P('stage')
- bias: float32 [16, 2048], P('stage')
- h_init: float32 [16, 1024, 512], P('stage', 'data'), parts along dimension 1
- c_init: float32 [16, 1024, 512], P('stage', 'data'), parts along dimension 1
Outputs:
- output 1: float32 [4], P('data'), parts along dimension 0
- output 2: float32 [64, 512, 2048], P(('data', 'stage')), parts along dimension 0
- output 3: float32 [64, 512, 2048], P(('data', 'stage')), parts along dimension 0
- output 4: float32 [64, 2048], P(('data', 'stage')), parts along dimension 0
- output 5: float32 [16, 1024, 512], P('stage', 'data'), parts along dimension 1
- output 6: float32 [16, 1024, 512], P('stage', 'data'), parts along dimension 1
There are 4 independent parts. The reference program is written for one: setup_inputs(seed, part) draws one part's arguments, and reference() takes and returns one part's arrays. A program takes and returns all parts, laid end to end along the dimension named above; an argument that names none is the same for every part.
All inputs are finite; a program needn't handle non-finite values.
Results may differ from the reference program's by a relative error of at most 0.0139054.
Values are sent between devices in bfloat16 or wider.
A program may use at most 768 MiB of HBM per device.

```python
import jax
import jax.numpy as jnp
from jax import lax

HIDDEN = 512
BATCH = 256
STEPS = 16
STAGES = 16
STAGE_LAYERS = 1
SEG_LEN = 16
LAYERS = STAGES * STAGE_LAYERS
NUM_SEGS = STEPS // SEG_LEN


def draw_lengths(key):
    len_key, row_key = jax.random.split(key)
    lengths = jax.random.randint(len_key, (BATCH,), STEPS // 4, STEPS + 1)
    full_row = jax.random.randint(row_key, (), 0, BATCH)
    return jnp.where(jnp.arange(BATCH) == full_row, STEPS, lengths).astype(jnp.int32)


def setup_inputs(seed: int = 0, part: int = 0) -> dict:
    shared = jax.random.split(jax.random.key(seed), 3)
    part_keys = jax.random.split(jax.random.fold_in(jax.random.key(seed + 1), part), 5)
    scale = HIDDEN ** -0.5
    gate_shift = jnp.concatenate([jnp.zeros((HIDDEN,), jnp.float32), jnp.ones((HIDDEN,), jnp.float32), jnp.zeros((2 * HIDDEN,), jnp.float32)])
    inputs = jax.random.normal(part_keys[0], (BATCH, STEPS, HIDDEN), jnp.float32)
    targets = 0.8 * jax.random.normal(part_keys[1], (BATCH, STEPS, HIDDEN), jnp.float32)
    w_in = 2.0 * scale * jax.random.normal(shared[0], (LAYERS, HIDDEN, 4 * HIDDEN), jnp.float32)
    w_rec = scale * jax.random.normal(shared[1], (LAYERS, HIDDEN, 4 * HIDDEN), jnp.float32)
    bias = 0.5 * jax.random.normal(shared[2], (LAYERS, 4 * HIDDEN), jnp.float32) + gate_shift
    h_init = 0.5 * jax.random.normal(part_keys[3], (LAYERS, BATCH, HIDDEN), jnp.float32)
    c_init = jax.random.normal(part_keys[4], (LAYERS, BATCH, HIDDEN), jnp.float32)
    return dict(inputs=inputs.astype(jnp.bfloat16), targets=targets.astype(jnp.bfloat16), lengths=draw_lengths(part_keys[2]), w_in=w_in.astype(jnp.bfloat16), w_rec=w_rec.astype(jnp.bfloat16), bias=bias, h_init=h_init, c_init=c_init)


def snap_bf16(value):
    return value + lax.stop_gradient(value.astype(jnp.bfloat16).astype(jnp.float32) - value)


def lstm_layer(layer_in, w_in, w_rec, bias, h_init, c_init, mask):
    seq_segs = layer_in.astype(jnp.float32).reshape(NUM_SEGS, SEG_LEN, BATCH, HIDDEN)
    mask_segs = mask.reshape(NUM_SEGS, SEG_LEN, BATCH, 1)

    def segment(state, seg_data):
        seg_in, seg_mask = seg_data
        in_proj = jnp.einsum('kbh,hg->kbg', seg_in, w_in) + bias

        def step(carry, step_data):
            h_prev, c_prev = carry
            proj_t, mask_t = step_data
            pre_act = proj_t + jnp.dot(h_prev, w_rec, preferred_element_type=jnp.float32)
            in_gate = jax.nn.sigmoid(pre_act[:, :HIDDEN])
            forget = jax.nn.sigmoid(pre_act[:, HIDDEN:2 * HIDDEN])
            candidate = jnp.tanh(pre_act[:, 2 * HIDDEN:3 * HIDDEN])
            out_gate = jax.nn.sigmoid(pre_act[:, 3 * HIDDEN:])
            c_cand = forget * c_prev + in_gate * candidate
            h_cand = snap_bf16(out_gate * jnp.tanh(c_cand))
            h_next = jnp.where(mask_t, h_cand, h_prev)
            c_next = jnp.where(mask_t, c_cand, c_prev)
            return (h_next, c_next), jnp.where(mask_t, h_cand, 0.0)

        return lax.scan(step, state, (in_proj, seg_mask))

    start = (snap_bf16(h_init), c_init)
    _, outputs = lax.scan(jax.checkpoint(segment), start, (seq_segs, mask_segs))
    return outputs.reshape(STEPS, BATCH, HIDDEN).astype(jnp.bfloat16)


def reference(inputs, targets, lengths, w_in, w_rec, bias, h_init, c_init):
    mask = (jnp.arange(STEPS)[:, None] < lengths[None, :])[:, :, None]
    first_seq = jnp.swapaxes(inputs, 0, 1)
    goal = jnp.swapaxes(targets, 0, 1).astype(jnp.float32)

    def total_loss(w_in_all, w_rec_all, bias_all, h_all, c_all):
        def layer_fn(layer_seq, layer_args):
            w_in_l, w_rec_l, bias_l, h_l, c_l = layer_args
            return lstm_layer(layer_seq, w_in_l, w_rec_l, bias_l, h_l, c_l, mask), None

        top_out, _ = lax.scan(jax.checkpoint(layer_fn), first_seq, (w_in_all, w_rec_all, bias_all, h_all, c_all))
        error = top_out.astype(jnp.float32) - goal
        return jnp.sum(jnp.where(mask, error * error, 0.0)) / (2.0 * BATCH * STEPS)

    loss, grads = jax.value_and_grad(total_loss, argnums=(0, 1, 2, 3, 4))(w_in.astype(jnp.float32), w_rec.astype(jnp.float32), bias, h_init, c_init)
    return (loss.reshape(1), grads[0], grads[1], grads[2], grads[3], grads[4])
```

```python
import functools

import jax
import jax.numpy as jnp
from jax import lax
from jax.experimental import pallas as pl
from jax.experimental.pallas import tpu as pltpu
from jax.sharding import PartitionSpec as P

F32 = jnp.float32
BF16 = jnp.bfloat16
W_STEPS = 4


def mm(lhs, rhs):
    return jnp.dot(lhs, rhs, preferred_element_type=F32)


def mm_t(lhs, rhs):
    return lax.dot_general(lhs, rhs, (((0,), (0,)), ((), ())), preferred_element_type=F32)


def sigmoid(value):
    return 0.5 * jnp.tanh(0.5 * value) + 0.5


def kernel(last, steps, rows, hidden,
           inputs_ref, targets_ref, lens_ref, w_in_ref, w_rec_ref, bias_ref, h0_ref, c0_ref,
           loss_ref, g_in_ref, g_rec_ref, g_bias_ref, dh0_ref, dc0_ref,
           gates, dz, hist, seq, dout, win, wrec, win_t, wrec_t, acc_in, acc_rec, ring_h, ring_d, dhs, dcs, lens,
           loss_acc, loss_buf, g_bias,
           f_recv, f_send, b_recv, b_send, loss_recv, loss_send, local_sem, out_sem):
    stage = lax.axis_index('stage')
    lo, hi = stage > 0, stage < last
    first, top = stage == 0, stage == last
    span = W_STEPS * rows
    batch = 2 * rows
    n_pieces = steps // W_STEPS
    scale = 1.0 / (batch * steps)

    def at_step(step):
        return pl.ds(pl.multiple_of(step * rows, rows), rows)

    def f_copy(group, step):
        slot = lax.rem(step, 2)
        return pltpu.make_async_remote_copy(
            src_ref=ring_h.at[group, slot], dst_ref=seq.at[group, at_step(step), :],
            send_sem=f_send.at[group, slot], recv_sem=f_recv.at[group, step],
            device_id={'stage': stage + 1}, device_id_type=pl.DeviceIdType.MESH)

    def b_copy(group, step):
        slot = lax.rem(step, 2)
        return pltpu.make_async_remote_copy(
            src_ref=ring_d.at[group, slot], dst_ref=dout.at[group, at_step(step), :],
            send_sem=b_send.at[group, slot], recv_sem=b_recv.at[group, step],
            device_id={'stage': stage - 1}, device_id_type=pl.DeviceIdType.MESH)

    def loss_copy():
        return pltpu.make_async_remote_copy(
            src_ref=loss_buf, dst_ref=loss_buf, send_sem=loss_send, recv_sem=loss_recv,
            device_id={'stage': stage - 1}, device_id_type=pl.DeviceIdType.MESH)

    def load(src, dst, sem):
        return pltpu.make_async_copy(src, dst, local_sem.at[sem])

    loads = []
    for q in range(4):
        cols = pl.ds(q * hidden, hidden)
        loads.append(load(w_in_ref.at[:, cols], win.at[q], 0 + q))
        loads.append(load(w_rec_ref.at[:, cols], wrec.at[q], 4 + q))
    loads.append(load(c0_ref.at[pl.ds(0, rows), :], dhs.at[1], 8))
    loads.append(load(c0_ref.at[pl.ds(rows, rows), :], dcs.at[1], 9))
    loads.append(load(c0_ref.at[pl.ds(0, rows), :], dhs.at[0], 10))
    loads.append(load(h0_ref.at[pl.ds(0, rows), :], gates.at[0, :, pl.ds(0, hidden)], 11))
    loads.append(load(h0_ref.at[pl.ds(rows, rows), :], gates.at[1, :, pl.ds(0, hidden)], 12))

    def land(src, group):
        return load(src.at[pl.ds(group * rows * steps, rows * steps), :],
                    dz.at[group, pl.ds(0, rows * steps), :], 13 + group)

    @pl.when(first)
    def _():
        for group in range(2):
            land(inputs_ref, group).start()

    for copy in loads:
        copy.start()

    @pl.when(top)
    def _():
        for group in range(2):
            land(targets_ref, group).start()

    barrier = pltpu.get_barrier_semaphore()

    @pl.when(lo)
    def _():
        pl.semaphore_signal(barrier, inc=1, device_id={'stage': stage - 1}, device_id_type=pl.DeviceIdType.MESH)

    @pl.when(hi)
    def _():
        pl.semaphore_signal(barrier, inc=1, device_id={'stage': stage + 1}, device_id_type=pl.DeviceIdType.MESH)

    for group in range(2):
        row = lens_ref[group:group + 1, :].astype(F32)
        lens[group] = jnp.broadcast_to(row, (128, rows)).T

    loss_acc[...] = jnp.zeros_like(loss_acc)
    g_bias[...] = jnp.zeros_like(g_bias)

    @pl.when(jnp.logical_and(lo, hi))
    def _():
        pl.semaphore_wait(barrier, 2)

    @pl.when(jnp.logical_or(first, top))
    def _():
        pl.semaphore_wait(barrier, 1)

    def time_major(group, dst):
        size = 16 * steps
        out_row = lax.broadcasted_iota(jnp.int32, (size, size), 0)
        in_row = lax.broadcasted_iota(jnp.int32, (size, size), 1)
        step_of, row_of = lax.div(out_row, 16), lax.rem(out_row, 16)
        permute = (in_row == row_of * steps + step_of).astype(F32).astype(BF16)

        def block(idx, _):
            piece = dz[group, pl.ds(pl.multiple_of(idx * size, size), size), :]
            moved = mm(permute, piece).astype(BF16)
            for step in range(steps):
                dst[group, pl.ds(pl.multiple_of(step * rows + idx * 16, 16), 16), :] = moved[step * 16:(step + 1) * 16]
            return 0

        lax.fori_loop(0, rows // 16, block, 0)

    def set_up():
        def turn(q, _):
            win_t[q] = win[q].T
            wrec_t[q] = wrec[q].T
            acc_in[q] = jnp.zeros((hidden, hidden), F32)
            acc_rec[q] = jnp.zeros((hidden, hidden), F32)
            return 0

        lax.fori_loop(0, 4, turn, 0)

    @pl.when(first)
    def _():
        land(inputs_ref, 0).wait()
        time_major(0, seq)

    for copy in loads:
        copy.wait()
    for group in range(2):
        h_start = gates[group, :, 0:hidden].astype(BF16)
        hist[group, 0:rows, :] = h_start
        ring_h[group, 1] = h_start

    @pl.when(top)
    def _():
        for group in range(2):
            land(targets_ref, group).wait()
            time_major(group, dout)

    early = stage >= (last + 1) // 2

    @pl.when(early)
    def _():
        set_up()

    def pre_act(x, h, q):
        return mm(x, win[q]) + mm(h, wrec[q]) + bias_ref[:, q * hidden:(q + 1) * hidden]

    def forward(group, step, c_ref):
        @pl.when(lo)
        def _():
            f_copy(group, step).wait_recv()

        slot = lax.rem(step, 2)
        x = seq[group, at_step(step), :]
        h = ring_h[group, 1 - slot]
        in_gate = sigmoid(pre_act(x, h, 0))
        cand = jnp.tanh(pre_act(x, h, 2))
        forget = sigmoid(pre_act(x, h, 1))
        c_new = forget * c_ref[...] + in_gate * cand
        c_ref[...] = c_new
        tanh_c = jnp.tanh(c_new)
        out_gate = sigmoid(pre_act(x, h, 3))
        live = jnp.tile(lens[group] > step.astype(F32), (1, hidden // 128))
        h_new = jnp.where(live, out_gate * tanh_c, 0.0).astype(BF16)

        @pl.when(jnp.logical_and(hi, step >= 2))
        def _():
            f_copy(group, step - 2).wait_send()

        ring_h[group, slot] = h_new

        @pl.when(hi)
        def _():
            f_copy(group, step).start()

        @pl.when(top)
        def _():
            goal = dout[group, at_step(step), :].astype(F32)
            out = ring_h[group, slot].astype(F32)
            now = jnp.tile(lens[group] > step.astype(F32), (1, hidden // 128))
            error = jnp.where(now, out - goal, 0.0)
            loss_acc[...] += jnp.sum((error * error).reshape(rows // 8, 8, hidden), axis=0)
            dout[group, at_step(step), :] = (error * scale).astype(BF16)

    def recompute(group, step, slot, c_ref):
        x = seq[group, at_step(step), :]
        h = hist[group, at_step(step), :]
        in_gate = sigmoid(pre_act(x, h, 0))
        gates[slot, :, 0:hidden] = in_gate
        cand = jnp.tanh(pre_act(x, h, 2))
        gates[slot, :, 2 * hidden:3 * hidden] = cand
        forget = sigmoid(pre_act(x, h, 1))
        gates[slot, :, hidden:2 * hidden] = forget
        c_prev = c_ref[...]
        gates[slot, :, 4 * hidden:5 * hidden] = c_prev
        c_new = forget * c_prev + in_gate * cand
        c_ref[...] = c_new
        out_gate = sigmoid(pre_act(x, h, 3))
        gates[slot, :, 3 * hidden:4 * hidden] = out_gate
        live = jnp.tile(lens[group] > step.astype(F32), (1, hidden // 128))
        hist[group, at_step(step + 1), :] = jnp.where(live, out_gate * jnp.tanh(c_new), 0.0).astype(BF16)

    def backward(group, step, slot, place):
        @pl.when(hi)
        def _():
            b_copy(group, step).wait_recv()

        d_h = dhs[group] + dout[group, at_step(step), :].astype(F32)
        in_gate = gates[slot, :, 0:hidden]
        forget = gates[slot, :, hidden:2 * hidden]
        cand = gates[slot, :, 2 * hidden:3 * hidden]
        out_gate = gates[slot, :, 3 * hidden:4 * hidden]
        c_prev = gates[slot, :, 4 * hidden:5 * hidden]
        tanh_c = jnp.tanh(forget * c_prev + in_gate * cand)
        d_cell = d_h * out_gate * (1.0 - tanh_c * tanh_c) + dcs[group]
        dcs[group] = d_cell * forget
        parts = [
            d_cell * cand * in_gate * (1.0 - in_gate),
            d_cell * c_prev * forget * (1.0 - forget),
            d_cell * in_gate * (1.0 - cand * cand),
            d_h * tanh_c * out_gate * (1.0 - out_gate)]
        low = []
        for q in range(4):
            g_bias[q] += jnp.sum(parts[q].reshape(rows // 8, 8, hidden), axis=0)
            low.append(parts[q].astype(BF16))
            dz[q, at_step(place), :] = low[q]
        ring_slot = lax.rem(step, 2)

        @pl.when(jnp.logical_and(lo, step < steps - 2))
        def _():
            b_copy(group, step + 2).wait_send()

        d_in = mm(low[0], win_t[0]) + mm(low[1], win_t[1]) + mm(low[2], win_t[2]) + mm(low[3], win_t[3])
        ring_d[group, ring_slot] = d_in.astype(BF16)

        @pl.when(lo)
        def _():
            b_copy(group, step).start()

        dhs[group] = mm(low[0], wrec_t[0]) + mm(low[1], wrec_t[1]) + mm(low[2], wrec_t[2]) + mm(low[3], wrec_t[3])

    def weight_piece(group, piece, q, place):
        here = pl.ds(pl.multiple_of(piece * span, span), span)
        there = pl.ds(pl.multiple_of(place * rows, span), span)
        d_part = dz[q, there, :]
        acc_in[q] += mm_t(seq[group, here, :], d_part)
        acc_rec[q] += mm_t(hist[group, here, :], d_part)

    def place_of(step):
        tick_piece = n_pieces - 1 - lax.div(step, W_STEPS)
        return lax.rem(tick_piece + n_pieces, n_pieces + 1) * W_STEPS + lax.rem(step, W_STEPS)

    def phase_1(step, _):
        forward(0, step, dhs.at[1])
        return 0

    lax.fori_loop(0, steps, phase_1, 0)

    @pl.when(first)
    def _():
        land(inputs_ref, 1).wait()
        time_major(1, seq)

    again = load(c0_ref.at[pl.ds(rows, rows), :], dhs.at[1], 8)
    again.start()

    def phase_2(step, _):
        recompute(0, step, step, dhs.at[0])
        forward(1, step, dcs.at[1])
        return 0

    lax.fori_loop(0, steps, phase_2, 0)
    again.wait()

    @pl.when(top)
    def _():
        total = jnp.sum(loss_acc[...]) * (0.5 * scale)
        loss_buf[...] = jnp.full(loss_buf.shape, total, F32)
        loss_copy().start()

    @pl.when(jnp.logical_not(early))
    def _():
        set_up()

    dhs[0] = jnp.zeros((rows, hidden), F32)
    dcs[0] = jnp.zeros((rows, hidden), F32)

    def phase_3(tick, _):
        recompute(1, tick, steps - tick, dhs.at[1])
        backward(0, steps - 1 - tick, steps - 1 - tick, steps - 1 - tick)
        return 0

    lax.fori_loop(0, steps, phase_3, 0)

    def put(src, dst, sem):
        return pltpu.make_async_copy(src, dst, out_sem.at[sem])

    stores = [put(dhs.at[0], dh0_ref.at[pl.ds(0, rows), :], 0), put(dcs.at[0], dc0_ref.at[pl.ds(0, rows), :], 1)]
    stores[0].start()
    stores[1].start()

    @pl.when(hi)
    def _():
        loss_copy().wait_recv()

        @pl.when(lo)
        def _():
            loss_copy().start()

    loss_ref[0] = loss_buf[0, 0]
    dhs[1] = jnp.zeros((rows, hidden), F32)
    dcs[1] = jnp.zeros((rows, hidden), F32)

    def phase_4(tick, _):
        step = steps - 1 - tick
        backward(1, step, steps - step, place_of(step))
        piece = lax.div(tick, W_STEPS)
        weight_piece(0, piece, lax.rem(tick, W_STEPS), piece * W_STEPS)
        return 0

    lax.fori_loop(0, steps, phase_4, 0)
    stores += [put(dhs.at[1], dh0_ref.at[pl.ds(rows, rows), :], 2), put(dcs.at[1], dc0_ref.at[pl.ds(rows, rows), :], 3)]
    stores[2].start()
    stores[3].start()
    for q in range(4):
        g_bias_ref[:, q * hidden:(q + 1) * hidden] = jnp.sum(g_bias[q], axis=0, keepdims=True)

    for q in range(4):
        def piece_loop(piece, _, q=q):
            weight_piece(1, piece, q, place_of(piece * W_STEPS))
            return 0

        lax.fori_loop(0, n_pieces, piece_loop, 0)
        cols = pl.ds(q * hidden, hidden)
        stores += [put(acc_in.at[q], g_in_ref.at[:, cols], 4 + 2 * q), put(acc_rec.at[q], g_rec_ref.at[:, cols], 5 + 2 * q)]
        stores[-2].start()
        stores[-1].start()

    for copy in stores:
        copy.wait()

    @pl.when(hi)
    def _():
        for group in range(2):
            for step in (steps - 2, steps - 1):
                f_copy(group, step).wait_send()

    @pl.when(lo)
    def _():
        for group in range(2):
            for step in (1, 0):
                b_copy(group, step).wait_send()
        loss_copy().wait_send()


def solution(mesh):
    last = mesh.shape['stage'] - 1

    def local(inputs, targets, lengths, w_in, w_rec, bias, h_init, c_init):
        batch, steps, hidden = inputs.shape
        rows = batch // 2
        wide = 4 * hidden
        any_spec = pl.BlockSpec(memory_space=pl.ANY)
        vmem_spec = pl.BlockSpec(memory_space=pltpu.VMEM)
        dma = pltpu.SemaphoreType.DMA
        loss, g_in, g_rec, g_bias, dh0, dc0 = pl.pallas_call(
            functools.partial(kernel, last, steps, rows, hidden),
            out_shape=(
                jax.ShapeDtypeStruct((1,), F32),
                jax.ShapeDtypeStruct((hidden, wide), F32),
                jax.ShapeDtypeStruct((hidden, wide), F32),
                jax.ShapeDtypeStruct((1, wide), F32),
                jax.ShapeDtypeStruct((batch, hidden), F32),
                jax.ShapeDtypeStruct((batch, hidden), F32)),
            in_specs=[any_spec, any_spec, vmem_spec, any_spec, any_spec, vmem_spec, any_spec, any_spec],
            out_specs=(pl.BlockSpec(memory_space=pltpu.SMEM), any_spec, any_spec, vmem_spec, any_spec, any_spec),
            scratch_shapes=[
                pltpu.VMEM((steps + 1, rows, 5 * hidden), F32),
                pltpu.VMEM((4, (steps + W_STEPS) * rows, hidden), BF16),
                pltpu.VMEM((2, (steps + 1) * rows, hidden), BF16),
                pltpu.VMEM((2, steps * rows, hidden), BF16),
                pltpu.VMEM((2, steps * rows, hidden), BF16),
                pltpu.VMEM((4, hidden, hidden), BF16),
                pltpu.VMEM((4, hidden, hidden), BF16),
                pltpu.VMEM((4, hidden, hidden), BF16),
                pltpu.VMEM((4, hidden, hidden), BF16),
                pltpu.VMEM((4, hidden, hidden), F32),
                pltpu.VMEM((4, hidden, hidden), F32),
                pltpu.VMEM((2, 2, rows, hidden), BF16),
                pltpu.VMEM((2, 2, rows, hidden), BF16),
                pltpu.VMEM((2, rows, hidden), F32),
                pltpu.VMEM((2, rows, hidden), F32),
                pltpu.VMEM((2, rows, 128), F32),
                pltpu.VMEM((8, hidden), F32),
                pltpu.VMEM((8, 128), F32),
                pltpu.VMEM((4, 8, hidden), F32),
                dma((2, steps)), dma((2, 2)), dma((2, steps)), dma((2, 2)), dma, dma, dma((15,)), dma((12,))],
            compiler_params=pltpu.CompilerParams(
                collective_id=0, has_side_effects=True, vmem_limit_bytes=67043328),
        )(inputs.reshape(batch * steps, hidden), targets.reshape(batch * steps, hidden), lengths.reshape(2, rows),
          w_in[0], w_rec[0], bias, h_init[0], c_init[0])
        return loss, g_in[None], g_rec[None], g_bias, dh0[None], dc0[None]

    layer_spec = P(('data', 'stage'))
    return jax.shard_map(
        local, mesh=mesh,
        in_specs=(P('data'), P('data'), P('data'), P('stage'), P('stage'), P('stage'), P('stage', 'data'), P('stage', 'data')),
        out_specs=(P('data'), layer_spec, layer_spec, layer_spec, P('stage', 'data'), P('stage', 'data')),
        check_vma=False)
```

```python
import functools

import jax
import jax.numpy as jnp
from jax import lax
from jax.experimental import pallas as pl
from jax.experimental.pallas import tpu as pltpu
from jax.sharding import PartitionSpec as P

F32 = jnp.float32
BF16 = jnp.bfloat16
COLS = 256
ROWS = 32
B_ROWS = 16
ORDER = (0, 2, 1, 3)
HELD_LIMIT = 47_700_000
FINISH_LIMIT = 16_000_000


def mm(lhs, rhs):
    return jnp.dot(lhs, rhs, preferred_element_type=F32)


def mm_t(lhs, rhs):
    return lax.dot_general(lhs, rhs, (((0,), (0,)), ((), ())), preferred_element_type=F32)


def sigmoid(value):
    return 0.5 * jnp.tanh(0.5 * value) + 0.5


def interleave(main, side):
    done = 0
    for idx, piece in enumerate(main):
        upto = (idx + 1) * len(side) // len(main)
        for other in side[done:upto]:
            other()
        done = upto
        piece()


def kernel(last, steps, rows, hidden,
           inputs_ref, targets_ref, lens_ref, w_in_ref, w_rec_ref, bias_ref, h0_ref, c0_ref,
           partial_ref, dz_1, hist, seq, dhs, dcs, g_bias, loss_buf,
           gates, dz_0, dout, win, wrec, win_t, wrec_t, ring_d, work, ahead, lens, loss_acc, fence,
           f_recv, f_send, b_recv, b_send, loss_recv, loss_send, local_sem, tile_sem):
    stage = lax.axis_index('stage')
    lo, hi = stage > 0, stage < last
    first, top = stage == 0, stage == last
    dz = (dz_0, dz_1)
    batch = 2 * rows
    scale = 1.0 / (batch * steps)

    def at_step(step):
        return pl.ds(pl.multiple_of(step * rows, rows), rows)

    def f_copy(group, step):
        slot = lax.rem(step, 2)
        return pltpu.make_async_remote_copy(
            src_ref=hist.at[group, at_step(steps + 1 + slot), :], dst_ref=seq.at[group, at_step(step), :],
            send_sem=f_send.at[group, slot], recv_sem=f_recv.at[group, step],
            device_id={'stage': stage + 1}, device_id_type=pl.DeviceIdType.MESH)

    def b_copy(group, step):
        slot = lax.rem(step, 2)
        return pltpu.make_async_remote_copy(
            src_ref=ring_d.at[group, slot], dst_ref=dout.at[group, at_step(step), :],
            send_sem=b_send.at[group, slot], recv_sem=b_recv.at[group, step],
            device_id={'stage': stage - 1}, device_id_type=pl.DeviceIdType.MESH)

    def loss_copy():
        return pltpu.make_async_remote_copy(
            src_ref=loss_buf, dst_ref=loss_buf, send_sem=loss_send, recv_sem=loss_recv,
            device_id={'stage': stage - 1}, device_id_type=pl.DeviceIdType.MESH)

    def load(src, dst, sem):
        return pltpu.make_async_copy(src, dst, local_sem.at[sem])

    loads = []
    for q in range(4):
        cols = pl.ds(q * hidden, hidden)
        loads.append(load(w_in_ref.at[:, cols], win.at[q], 0 + q))
        loads.append(load(w_rec_ref.at[:, cols], wrec.at[q], 4 + q))
    loads.append(load(c0_ref.at[pl.ds(0, rows), :], dhs.at[1], 8))
    loads.append(load(c0_ref.at[pl.ds(rows, rows), :], dcs.at[1], 9))
    loads.append(load(c0_ref.at[pl.ds(0, rows), :], dhs.at[0], 10))
    loads.append(load(h0_ref.at[pl.ds(0, rows), :], gates.at[0, :, pl.ds(0, hidden)], 11))
    loads.append(load(h0_ref.at[pl.ds(rows, rows), :], gates.at[1, :, pl.ds(0, hidden)], 12))

    def land(src, group):
        return load(src.at[pl.ds(group * rows * steps, rows * steps), :],
                    dz_0.at[group], 13 + group)

    @pl.when(first)
    def _():
        for group in range(2):
            land(inputs_ref, group).start()

    for copy in loads:
        copy.start()

    @pl.when(top)
    def _():
        for group in range(2):
            land(targets_ref, group).start()

    barrier = pltpu.get_barrier_semaphore()

    @pl.when(lo)
    def _():
        pl.semaphore_signal(barrier, inc=1, device_id={'stage': stage - 1}, device_id_type=pl.DeviceIdType.MESH)

    @pl.when(hi)
    def _():
        pl.semaphore_signal(barrier, inc=1, device_id={'stage': stage + 1}, device_id_type=pl.DeviceIdType.MESH)

    for group in range(2):
        row = lens_ref[group:group + 1, :].astype(F32)
        lens[group] = jnp.broadcast_to(row, (128, rows)).T

    loss_acc[...] = jnp.zeros_like(loss_acc)
    g_bias[...] = jnp.zeros_like(g_bias)

    @pl.when(jnp.logical_and(lo, hi))
    def _():
        pl.semaphore_wait(barrier, 2)

    @pl.when(jnp.logical_or(first, top))
    def _():
        pl.semaphore_wait(barrier, 1)

    def time_major(group, dst):
        size = 16 * steps
        out_row = lax.broadcasted_iota(jnp.int32, (size, size), 0)
        in_row = lax.broadcasted_iota(jnp.int32, (size, size), 1)
        step_of, row_of = lax.div(out_row, 16), lax.rem(out_row, 16)
        permute = (in_row == row_of * steps + step_of).astype(F32).astype(BF16)

        def block(idx, _):
            piece = dz_0[group, pl.ds(pl.multiple_of(idx * size, size), size), :]
            moved = mm(permute, piece).astype(BF16)
            for step in range(steps):
                dst[group, pl.ds(pl.multiple_of(step * rows + idx * 16, 16), 16), :] = moved[step * 16:(step + 1) * 16]
            return 0

        lax.fori_loop(0, rows // 16, block, 0)

    def set_up():
        def turn(q, _):
            win_t[q] = win[q].T
            wrec_t[q] = wrec[q].T
            return 0

        lax.fori_loop(0, 4, turn, 0)

    @pl.when(first)
    def _():
        land(inputs_ref, 0).wait()
        time_major(0, seq)

    for copy in loads:
        copy.wait()
    for group in range(2):
        h_start = gates[group, :, 0:hidden].astype(BF16)
        hist[group, 0:rows, :] = h_start
        hist[group, (steps + 2) * rows:(steps + 3) * rows, :] = h_start

    @pl.when(top)
    def _():
        for group in range(2):
            land(targets_ref, group).wait()
            time_major(group, dout)

    early = stage >= (last + 1) // 2

    @pl.when(early)
    def _():
        set_up()

    def cols_of(block):
        return slice(block * COLS, (block + 1) * COLS)

    def bias_of(q, block):
        return bias_ref[:, q * hidden + block * COLS:q * hidden + (block + 1) * COLS]

    def cell(group, step, z, c_ref, rs, cs, slot=None):
        in_gate, cand = sigmoid(z[0]), jnp.tanh(z[2])
        forget = sigmoid(z[1])
        c_prev = c_ref[rs, cs]
        c_new = forget * c_prev + in_gate * cand
        c_ref[rs, cs] = c_new
        out_gate = sigmoid(z[3])
        if slot is not None:
            for part, value in enumerate((in_gate, forget, cand, out_gate, c_prev)):
                gates[slot, rs, part * hidden + cs.start:part * hidden + cs.stop] = value
        live = jnp.tile(lens[group, rs, :] > step.astype(F32), (1, COLS // 128))
        return jnp.where(live, out_gate * jnp.tanh(c_new), 0.0).astype(BF16)

    def row_blocks():
        return [slice(r, r + ROWS) for r in range(0, rows, ROWS)]

    def forward_old(group, step):
        def piece(block, q):
            cs = cols_of(block)
            h = hist[group, at_step(steps + 2 - lax.rem(step, 2)), :]
            work[:, q * hidden + cs.start:q * hidden + cs.stop] = mm(h, wrec[q, :, cs]) + bias_of(q, block)

        return [functools.partial(piece, block, q) for block in range(hidden // COLS) for q in ORDER]

    def forward_wait(group, step):
        @pl.when(lo)
        def _():
            f_copy(group, step).wait_recv()
            fence[...] = jnp.zeros_like(fence)

        @pl.when(jnp.logical_and(hi, step >= 2))
        def _():
            f_copy(group, step - 2).wait_send()

    def forward_new(group, step, c_ref):
        slot = lax.rem(step, 2)
        x = seq[group, at_step(step), :]
        for block in range(hidden // COLS):
            cs = cols_of(block)
            new = {q: mm(x, win[q, :, cs]) for q in ORDER}
            for rs in row_blocks():
                z = [new[q][rs] + work[rs, q * hidden + cs.start:q * hidden + cs.stop] for q in range(4)]
                at = pl.ds(pl.multiple_of((steps + 1 + slot) * rows + rs.start, ROWS), ROWS)
                hist[group, at, cs] = cell(group, step, z, c_ref, rs, cs)

    def forward_send(group, step):
        @pl.when(hi)
        def _():
            f_copy(group, step).start()

        @pl.when(top)
        def _():
            slot = lax.rem(step, 2)
            for rs in row_blocks():
                at = pl.ds(pl.multiple_of(step * rows + rs.start, ROWS), ROWS)
                live = jnp.tile(lens[group, rs, :] > step.astype(F32), (1, hidden // 128))
                error = jnp.where(live, hist[group, pl.ds(pl.multiple_of((steps + 1 + slot) * rows + rs.start, ROWS), ROWS), :].astype(F32) - dout[group, at, :].astype(F32), 0.0)
                loss_acc[...] += jnp.sum((error * error).reshape(ROWS // 8, 8, hidden), axis=0)
                dout[group, at, :] = (error * scale).astype(BF16)

    def recompute_mm(group, step):
        def piece(block, q):
            cs = cols_of(block)
            x = seq[group, at_step(step), :]
            h = hist[group, at_step(step), :]
            ahead[:, q * hidden + cs.start:q * hidden + cs.stop] = mm(x, win[q, :, cs]) + mm(h, wrec[q, :, cs])

        return [functools.partial(piece, block, q) for block in range(hidden // COLS) for q in ORDER]

    def recompute_cell(group, step, slot, c_ref):
        def piece(block, rs):
            cs = cols_of(block)
            z = [ahead[rs, q * hidden + cs.start:q * hidden + cs.stop] + bias_of(q, block) for q in range(4)]
            at = pl.ds(pl.multiple_of((step + 1) * rows + rs.start, ROWS), ROWS)
            hist[group, at, cs] = cell(group, step, z, c_ref, rs, cs, slot)

        return [functools.partial(piece, block, rs) for block in range(hidden // COLS) for rs in row_blocks()]

    def backward_wait(group, step):
        @pl.when(hi)
        def _():
            b_copy(group, step).wait_recv()
            fence[...] = jnp.zeros_like(fence)

        @pl.when(jnp.logical_and(lo, step < steps - 2))
        def _():
            b_copy(group, step + 2).wait_send()

    def factors(slot):
        def piece(block, r):
            cs = cols_of(block)
            rs = slice(r, r + B_ROWS)
            in_gate, forget, cand, out_gate, c_prev = [
                gates[slot, rs, part * hidden + cs.start:part * hidden + cs.stop] for part in range(5)]
            new, old = in_gate * cand, forget * c_prev
            tanh_c = jnp.tanh(old + new)
            out = out_gate * tanh_c
            values = (new * (1.0 - in_gate), old * (1.0 - forget), in_gate - new * cand, out * (1.0 - out_gate),
                      out_gate - out * tanh_c, forget)
            for part, value in enumerate(values):
                work[rs, part * hidden + cs.start:part * hidden + cs.stop] = value

        return [functools.partial(piece, block, r) for block in range(hidden // COLS) for r in range(0, rows, B_ROWS)]

    def now_rows(q, start, stop):
        base = (steps + 3 + q % 2) * rows
        return slice(base + start, base + stop)

    def backward_cell(group, step):
        for block in range(hidden // COLS):
            cs = cols_of(block)
            sums = [None] * 4
            for r in range(0, rows, B_ROWS):
                rs = slice(r, r + B_ROWS)
                at = pl.ds(pl.multiple_of(step * rows + r, B_ROWS), B_ROWS)
                f = [work[rs, part * hidden + cs.start:part * hidden + cs.stop] for part in range(6)]
                d_h = dhs[group, rs, cs] + dout[group, at, cs].astype(F32)
                d_cell = d_h * f[4] + dcs[group, rs, cs]
                dcs[group, rs, cs] = d_cell * f[5]
                for q, value in enumerate((d_cell * f[0], d_cell * f[1], d_cell * f[2], d_h * f[3])):
                    low = value.astype(BF16)
                    hist[q // 2, now_rows(q, r, r + B_ROWS), cs] = low
                    dz[group][q, at, cs] = low
                    part = jnp.sum(value.reshape(B_ROWS // 8, 8, COLS), axis=0)
                    sums[q] = part if sums[q] is None else sums[q] + part
            for q in range(4):
                g_bias[q, :, cs] += sums[q]

    def through(weights, store):
        held = [None]
        n_blocks = hidden // COLS

        def piece(block, q):
            part = mm(hist[q // 2, now_rows(q, 0, rows), cols_of(block)], weights[q, cols_of(block), :])
            held[0] = part if held[0] is None else held[0] + part
            if block == n_blocks - 1 and q == 3:
                store(held[0])

        return [functools.partial(piece, block, q) for block in range(n_blocks) for q in range(4)]

    def backward_state(group):
        def store(value):
            dhs[group] = value

        return through(wrec_t, store)

    def backward_mm(group, step):
        def store(value):
            ring_d[group, lax.rem(step, 2)] = value.astype(BF16)

        for piece in through(win_t, store):
            piece()

    def backward_send(group, step):
        @pl.when(lo)
        def _():
            b_copy(group, step).start()

    def weight_tile(group, tick):
        q, m = lax.div(tick, 4), lax.rem(tick, 4)
        across = pl.ds(pl.multiple_of(m * (hidden // 4), hidden // 4), hidden // 4)

        def piece(which):
            lhs = seq[group, :, across] if which == 0 else hist[group, 0:steps * rows, across]
            gates[tick, :, which * hidden:(which + 1) * hidden] = mm_t(lhs, dz[group][q])

        return [functools.partial(piece, which) for which in range(2)]

    def tile_copy(tick, which):
        q, m = lax.div(tick, 4), lax.rem(tick, 4)
        part = hidden // 4
        return pltpu.make_async_copy(
            gates.at[tick, :, pl.ds(which * hidden, hidden)],
            partial_ref.at[which, pl.ds(pl.multiple_of(m * part, part), part), pl.ds(pl.multiple_of(q * hidden, hidden), hidden)],
            tile_sem.at[which, tick])

    def phase_1(step, _):
        interleave(forward_old(0, step), [])
        forward_wait(0, step)
        forward_new(0, step, dhs.at[1])
        forward_send(0, step)
        return 0

    lax.fori_loop(0, steps, phase_1, 0)

    @pl.when(first)
    def _():
        land(inputs_ref, 1).wait()
        time_major(1, seq)

    again = load(c0_ref.at[pl.ds(rows, rows), :], dhs.at[1], 8)
    again.start()

    def phase_2(step, _):
        interleave(forward_old(1, step), recompute_cell(0, step, step, dhs.at[0]))
        ahead_step = step + 1
        interleave(recompute_mm(lax.div(ahead_step, steps), lax.rem(ahead_step, steps)), [])
        forward_wait(1, step)
        forward_new(1, step, dcs.at[1])
        forward_send(1, step)
        return 0

    interleave(recompute_mm(0, 0), [])
    lax.fori_loop(0, steps, phase_2, 0)
    again.wait()

    @pl.when(top)
    def _():
        total = jnp.sum(loss_acc[...]) * (0.5 * scale)
        loss_buf[...] = jnp.full(loss_buf.shape, total, F32)
        loss_copy().start()

    @pl.when(jnp.logical_not(early))
    def _():
        set_up()

    dcs[0] = jnp.zeros((rows, hidden), F32)
    for q in range(4):
        hist[q // 2, now_rows(q, 0, rows), :] = jnp.zeros((rows, hidden), BF16)

    def phase_3(tick, _):
        step = steps - 1 - tick
        interleave(backward_state(0), recompute_cell(1, tick, steps - tick, dhs.at[1]))
        interleave(recompute_mm(1, lax.rem(tick + 1, steps)), factors(step))
        backward_wait(0, step)
        backward_cell(0, step)
        backward_mm(0, step)
        backward_send(0, step)
        return 0

    lax.fori_loop(0, steps, phase_3, 0)
    interleave(backward_state(0), [])

    @pl.when(hi)
    def _():
        loss_copy().wait_recv()

        @pl.when(lo)
        def _():
            loss_copy().start()

    dcs[1] = jnp.zeros((rows, hidden), F32)
    for q in range(4):
        hist[q // 2, now_rows(q, 0, rows), :] = jnp.zeros((rows, hidden), BF16)

    def phase_4(tick, _):
        step = steps - 1 - tick

        @pl.when(tick > 0)
        def _():
            for which in range(2):
                tile_copy(tick - 1, which).start()

        interleave(backward_state(1), factors(steps - step))
        interleave(weight_tile(0, tick), [])
        backward_wait(1, step)
        backward_cell(1, step)
        backward_mm(1, step)
        backward_send(1, step)
        return 0

    lax.fori_loop(0, steps, phase_4, 0)
    interleave(backward_state(1), [])
    for which in range(2):
        tile_copy(steps - 1, which).start()

    def tile_wait(tick, _):
        for which in range(2):
            tile_copy(tick, which).wait()
        return 0

    lax.fori_loop(0, steps, tile_wait, 0)

    @pl.when(hi)
    def _():
        for group in range(2):
            for step in (steps - 2, steps - 1):
                f_copy(group, step).wait_send()

    @pl.when(lo)
    def _():
        for group in range(2):
            for step in (1, 0):
                b_copy(group, step).wait_send()
        loss_copy().wait_send()


def finish_kernel(steps, rows, hidden, partial_ref, dz, hist, seq, dhs, dcs, g_bias, loss_buf,
                  loss_ref, g_in_ref, g_rec_ref, g_bias_ref, dh0_ref, dc0_ref, total, in_sem, out_sem, state_sem):
    def take(q, which):
        cols = pl.ds(pl.multiple_of(q * hidden, hidden), hidden)
        return pltpu.make_async_copy(partial_ref.at[which, :, cols], total.at[q, which], in_sem.at[q, which])

    def put(q, which):
        cols = pl.ds(pl.multiple_of(q * hidden, hidden), hidden)
        return pltpu.make_async_copy(total.at[q, which], (g_in_ref, g_rec_ref)[which].at[:, cols], out_sem.at[q, which])

    for q in range(4):
        for which in range(2):
            take(q, which).start()
    states = []
    for group in range(2):
        at = pl.ds(group * rows, rows)
        states.append(pltpu.make_async_copy(dhs.at[group], dh0_ref.at[at, :], state_sem.at[group]))
        states.append(pltpu.make_async_copy(dcs.at[group], dc0_ref.at[at, :], state_sem.at[2 + group]))
    for copy in states:
        copy.start()
    loss_ref[0] = loss_buf[0, 0]
    for q in range(4):
        g_bias_ref[:, q * hidden:(q + 1) * hidden] = jnp.sum(g_bias[q], axis=0, keepdims=True)

    def gate(q, _):
        new = [mm_t(lhs, dz[q]) for lhs in (seq[1], hist[1, 0:steps * rows, :])]
        for which in range(2):
            take(q, which).wait()
        for which in range(2):
            total[q, which] = total[q, which] + new[which]
            put(q, which).start()
        return 0

    lax.fori_loop(0, 4, gate, 0)
    for copy in states:
        copy.wait()
    for q in range(4):
        for which in range(2):
            put(q, which).wait()


def solution(mesh):
    last = mesh.shape['stage'] - 1

    def local(inputs, targets, lengths, w_in, w_rec, bias, h_init, c_init):
        batch, steps, hidden = inputs.shape
        rows = batch // 2
        wide = 4 * hidden
        any_spec = pl.BlockSpec(memory_space=pl.ANY)
        vmem_spec = pl.BlockSpec(memory_space=pltpu.VMEM)
        dma = pltpu.SemaphoreType.DMA
        held = pl.pallas_call(
            functools.partial(kernel, last, steps, rows, hidden),
            out_shape=(
                jax.ShapeDtypeStruct((8, hidden, wide), F32),
                pltpu.VMEM((4, steps * rows, hidden), BF16),
                pltpu.VMEM((2, (steps + 5) * rows, hidden), BF16),
                pltpu.VMEM((2, steps * rows, hidden), BF16),
                pltpu.VMEM((2, rows, hidden), F32),
                pltpu.VMEM((2, rows, hidden), F32),
                pltpu.VMEM((4, 8, hidden), F32),
                pltpu.VMEM((8, 128), F32)),
            in_specs=[any_spec, any_spec, vmem_spec, any_spec, any_spec, vmem_spec, any_spec, any_spec],
            out_specs=(any_spec,) + (vmem_spec,) * 7,
            scratch_shapes=[
                pltpu.VMEM((steps + 1, rows, 5 * hidden), F32),
                pltpu.VMEM((4, steps * rows, hidden), BF16),
                pltpu.VMEM((2, steps * rows, hidden), BF16),
                pltpu.VMEM((4, hidden, hidden), BF16),
                pltpu.VMEM((4, hidden, hidden), BF16),
                pltpu.VMEM((4, hidden, hidden), BF16),
                pltpu.VMEM((4, hidden, hidden), BF16),
                pltpu.VMEM((2, 2, rows, hidden), BF16),
                pltpu.VMEM((rows, 6 * hidden), F32),
                pltpu.VMEM((rows, 4 * hidden), F32),
                pltpu.VMEM((2, rows, 128), F32),
                pltpu.VMEM((8, hidden), F32),
                pltpu.VMEM((8, 128), F32),
                dma((2, steps)), dma((2, 2)), dma((2, steps)), dma((2, 2)), dma, dma, dma((15,)), dma((2, steps))],
            compiler_params=pltpu.CompilerParams(
                collective_id=0, has_side_effects=True, vmem_limit_bytes=HELD_LIMIT),
        )(inputs.reshape(batch * steps, hidden), targets.reshape(batch * steps, hidden), lengths.reshape(2, rows),
          w_in[0], w_rec[0], bias, h_init[0], c_init[0])
        loss, g_in, g_rec, g_bias, dh0, dc0 = pl.pallas_call(
            functools.partial(finish_kernel, steps, rows, hidden),
            out_shape=(
                jax.ShapeDtypeStruct((1,), F32),
                jax.ShapeDtypeStruct((hidden, wide), F32),
                jax.ShapeDtypeStruct((hidden, wide), F32),
                jax.ShapeDtypeStruct((1, wide), F32),
                jax.ShapeDtypeStruct((batch, hidden), F32),
                jax.ShapeDtypeStruct((batch, hidden), F32)),
            in_specs=[pl.BlockSpec(memory_space=pltpu.HBM)] + [vmem_spec] * 7,
            out_specs=(pl.BlockSpec(memory_space=pltpu.SMEM), any_spec, any_spec, vmem_spec, any_spec, any_spec),
            scratch_shapes=[pltpu.VMEM((4, 2, hidden, hidden), F32), dma((4, 2)), dma((4, 2)), dma((4,))],
            compiler_params=pltpu.CompilerParams(vmem_limit_bytes=FINISH_LIMIT),
        )(*held)
        return loss, g_in[None], g_rec[None], g_bias, dh0[None], dc0[None]

    layer_spec = P(('data', 'stage'))
    return jax.shard_map(
        local, mesh=mesh,
        in_specs=(P('data'), P('data'), P('data'), P('stage'), P('stage'), P('stage'), P('stage', 'data'), P('stage', 'data')),
        out_specs=(P('data'), layer_spec, layer_spec, layer_spec, P('stage', 'data'), P('stage', 'data')),
        check_vma=False)
```

```python
import functools

import jax
import jax.numpy as jnp
from jax import lax
from jax.experimental import pallas as pl
from jax.experimental.pallas import tpu as pltpu
from jax.sharding import PartitionSpec as P

F32 = jnp.float32
BF16 = jnp.bfloat16
COLS = 256
ROWS = 32
B_ROWS = 16
ORDER = (0, 2, 1, 3)
HELD_LIMIT = 48_700_000
FINISH_LIMIT = 16_000_000


def mm(lhs, rhs):
    return jnp.dot(lhs, rhs, preferred_element_type=F32)


def mm_t(lhs, rhs):
    return lax.dot_general(lhs, rhs, (((0,), (0,)), ((), ())), preferred_element_type=F32)


def sigmoid(value):
    return 0.5 * jnp.tanh(0.5 * value) + 0.5


def interleave(main, side):
    done = 0
    for idx, piece in enumerate(main):
        upto = (idx + 1) * len(side) // len(main)
        for other in side[done:upto]:
            other()
        done = upto
        piece()


def kernel(last, steps, rows, hidden,
           inputs_ref, targets_ref, lens_ref, w_in_ref, w_rec_ref, bias_ref, h0_ref, c0_ref,
           partial_ref, dz_1, hist, seq, dhs, dcs, g_bias, loss_buf,
           gates, dz_0, now, dout, win_t, wrec_t, ring_h, ring_d, work, lens, loss_acc, fence,
           f_recv, f_send, b_recv, b_send, loss_recv, loss_send, local_sem, tile_sem):
    stage = lax.axis_index('stage')
    lo, hi = stage > 0, stage < last
    first, top = stage == 0, stage == last
    dz = (dz_0, dz_1)
    win, wrec = dz_1.at[:, pl.ds(0, hidden), :], dz_1.at[:, pl.ds(hidden, hidden), :]
    batch = 2 * rows
    scale = 1.0 / (batch * steps)

    def at_step(step):
        return pl.ds(pl.multiple_of(step * rows, rows), rows)

    def f_copy(group, step):
        slot = lax.rem(step, 2)
        return pltpu.make_async_remote_copy(
            src_ref=ring_h.at[group, slot], dst_ref=seq.at[group, at_step(step), :],
            send_sem=f_send.at[group, slot], recv_sem=f_recv.at[group, step],
            device_id={'stage': stage + 1}, device_id_type=pl.DeviceIdType.MESH)

    def b_copy(group, step):
        slot = lax.rem(step, 2)
        return pltpu.make_async_remote_copy(
            src_ref=ring_d.at[group, slot], dst_ref=dout.at[group, at_step(step), :],
            send_sem=b_send.at[group, slot], recv_sem=b_recv.at[group, step],
            device_id={'stage': stage - 1}, device_id_type=pl.DeviceIdType.MESH)

    def loss_copy():
        return pltpu.make_async_remote_copy(
            src_ref=loss_buf, dst_ref=loss_buf, send_sem=loss_send, recv_sem=loss_recv,
            device_id={'stage': stage - 1}, device_id_type=pl.DeviceIdType.MESH)

    def load(src, dst, sem):
        return pltpu.make_async_copy(src, dst, local_sem.at[sem])

    loads = []
    for q in range(4):
        cols = pl.ds(q * hidden, hidden)
        loads.append(load(w_in_ref.at[:, cols], win.at[q], 0 + q))
        loads.append(load(w_rec_ref.at[:, cols], wrec.at[q], 4 + q))
    loads.append(load(c0_ref.at[pl.ds(0, rows), :], dhs.at[1], 8))
    loads.append(load(c0_ref.at[pl.ds(rows, rows), :], dcs.at[1], 9))
    loads.append(load(c0_ref.at[pl.ds(0, rows), :], dhs.at[0], 10))
    loads.append(load(h0_ref.at[pl.ds(0, rows), :], gates.at[0, :, pl.ds(0, hidden)], 11))
    loads.append(load(h0_ref.at[pl.ds(rows, rows), :], gates.at[1, :, pl.ds(0, hidden)], 12))

    def land(src, group):
        return load(src.at[pl.ds(group * rows * steps, rows * steps), :],
                    dz_0.at[group], 13 + group)

    @pl.when(first)
    def _():
        land(inputs_ref, 0).start()

    for copy in loads:
        copy.start()

    @pl.when(first)
    def _():
        land(inputs_ref, 1).start()

    @pl.when(top)
    def _():
        for group in range(2):
            land(targets_ref, group).start()

    barrier = pltpu.get_barrier_semaphore()

    @pl.when(lo)
    def _():
        pl.semaphore_signal(barrier, inc=1, device_id={'stage': stage - 1}, device_id_type=pl.DeviceIdType.MESH)

    @pl.when(hi)
    def _():
        pl.semaphore_signal(barrier, inc=1, device_id={'stage': stage + 1}, device_id_type=pl.DeviceIdType.MESH)

    for group in range(2):
        row = lens_ref[group:group + 1, :].astype(F32)
        lens[group] = jnp.broadcast_to(row, (128, rows)).T

    loss_acc[...] = jnp.zeros_like(loss_acc)
    g_bias[...] = jnp.zeros_like(g_bias)

    @pl.when(jnp.logical_and(lo, hi))
    def _():
        pl.semaphore_wait(barrier, 2)

    @pl.when(jnp.logical_or(first, top))
    def _():
        pl.semaphore_wait(barrier, 1)

    def time_major(group, dst):
        size = 16 * steps
        out_row = lax.broadcasted_iota(jnp.int32, (size, size), 0)
        in_row = lax.broadcasted_iota(jnp.int32, (size, size), 1)
        step_of, row_of = lax.div(out_row, 16), lax.rem(out_row, 16)
        permute = (in_row == row_of * steps + step_of).astype(F32).astype(BF16)

        def blocks(trip, _):
            for idx in (trip * 2, trip * 2 + 1):
                piece = dz_0[group, pl.ds(pl.multiple_of(idx * size, size), size), :]
                moved = mm(permute, piece).astype(BF16)
                for step in range(steps):
                    dst[group, pl.ds(pl.multiple_of(step * rows + idx * 16, 16), 16), :] = moved[step * 16:(step + 1) * 16]
            return 0

        lax.fori_loop(0, rows // 32, blocks, 0)

    def set_up():
        def turn(q, _):
            win_t[q] = win[q].T
            wrec_t[q] = wrec[q].T
            return 0

        lax.fori_loop(0, 4, turn, 0)

    @pl.when(first)
    def _():
        land(inputs_ref, 0).wait()
        time_major(0, seq)

    for copy in loads:
        copy.wait()
    for group in range(2):
        h_start = gates[group, :, 0:hidden].astype(BF16)
        hist[group, 0:rows, :] = h_start
        ring_h[group, 1] = h_start

    @pl.when(top)
    def _():
        for group in range(2):
            land(targets_ref, group).wait()
            time_major(group, dout)

    early = stage >= (last + 1) // 2

    @pl.when(early)
    def _():
        set_up()

    def cols_of(block):
        return slice(block * COLS, (block + 1) * COLS)

    def bias_of(q, block):
        return bias_ref[:, q * hidden + block * COLS:q * hidden + (block + 1) * COLS]

    def cell(group, step, z, c_ref, rs, cs, slot=None):
        in_gate, cand = sigmoid(z[0]), jnp.tanh(z[2])
        forget = sigmoid(z[1])
        new, old = in_gate * cand, forget * c_ref[rs, cs]
        c_new = old + new
        c_ref[rs, cs] = c_new
        tanh_c = jnp.tanh(c_new)
        out_gate = sigmoid(z[3])
        out = out_gate * tanh_c
        if slot is not None:
            values = (new * (1.0 - in_gate), old * (1.0 - forget), in_gate - new * cand, out * (1.0 - out_gate),
                      out_gate - out * tanh_c, forget)
            for part, value in enumerate(values):
                gates[slot, rs, part * hidden + cs.start:part * hidden + cs.stop] = value
        live = jnp.tile(lens[group, rs, :] > step.astype(F32), (1, COLS // 128))
        return jnp.where(live, out, 0.0).astype(BF16)

    def row_blocks():
        return [slice(r, r + ROWS) for r in range(0, rows, ROWS)]

    def forward_old(group, step):
        def piece(q):
            h = ring_h[group, 1 - lax.rem(step, 2)]
            at = slice(q * hidden, (q + 1) * hidden)
            work[:, at] = mm(h, wrec[q]) + bias_ref[:, at]

        return [functools.partial(piece, q) for q in ORDER]

    def forward_wait(group, step):
        @pl.when(lo)
        def _():
            f_copy(group, step).wait_recv()
            fence[...] = jnp.zeros_like(fence)

        @pl.when(jnp.logical_and(hi, step >= 2))
        def _():
            f_copy(group, step - 2).wait_send()

    def forward_new(group, step, c_ref):
        slot = lax.rem(step, 2)
        x = seq[group, at_step(step), :]
        n_blocks = hidden // COLS
        order = [(q, block) for block in range(n_blocks) for q in (0, 1, 2)] + [(3, block) for block in range(n_blocks)]
        new = {(q, block): mm(x, win[q, :, cols_of(block)]) for q, block in order}
        bent = {}

        def z(q, block, rs):
            return new[q, block][rs] + work[rs, q * hidden + block * COLS:q * hidden + (block + 1) * COLS]

        for block in range(n_blocks):
            cs = cols_of(block)
            for rs in row_blocks():
                in_gate, cand, forget = sigmoid(z(0, block, rs)), jnp.tanh(z(2, block, rs)), sigmoid(z(1, block, rs))
                c_new = forget * c_ref[rs, cs] + in_gate * cand
                c_ref[rs, cs] = c_new
                bent[block, rs.start] = jnp.tanh(c_new)
        for block in range(n_blocks):
            for rs in row_blocks():
                live = jnp.tile(lens[group, rs, :] > step.astype(F32), (1, COLS // 128))
                out = sigmoid(z(3, block, rs)) * bent[block, rs.start]
                ring_h[group, slot, rs, cols_of(block)] = jnp.where(live, out, 0.0).astype(BF16)

    def forward_send(group, step):
        @pl.when(hi)
        def _():
            f_copy(group, step).start()

        if group == 0:
            @pl.when(top)
            def _():
                output_error(group, step, lambda rs: ring_h[group, lax.rem(step, 2), rs, :])

    def output_error(group, step, made):
        for rs in row_blocks():
            at = pl.ds(pl.multiple_of(step * rows + rs.start, ROWS), ROWS)
            live = jnp.tile(lens[group, rs, :] > step.astype(F32), (1, hidden // 128))
            error = jnp.where(live, made(rs).astype(F32) - dout[group, at, :].astype(F32), 0.0)
            loss_acc[...] += jnp.sum((error * error).reshape(ROWS // 8, 8, hidden), axis=0)
            dout[group, at, :] = (error * scale).astype(BF16)

    def recompute_mm(group, step):
        x = seq[group, at_step(step), :]
        h = hist[group, at_step(step), :]
        return [{q: mm(x, win[q, :, cols_of(block)]) + mm(h, wrec[q, :, cols_of(block)]) for q in ORDER}
                for block in range(hidden // COLS)]

    def recompute_cell(group, step, slot, c_ref, new, block):
        cs = cols_of(block)
        for rs in row_blocks():
            z = [new[block][q][rs] + bias_of(q, block) for q in range(4)]
            at = pl.ds(pl.multiple_of((step + 1) * rows + rs.start, ROWS), ROWS)
            hist[group, at, cs] = cell(group, step, z, c_ref, rs, cs, slot)

    def backward_wait(group, step):
        @pl.when(hi)
        def _():
            b_copy(group, step).wait_recv()
            fence[...] = jnp.zeros_like(fence)

        if group == 1:
            @pl.when(top)
            def _():
                output_error(group, step, lambda rs: hist[
                    group, pl.ds(pl.multiple_of((step + 1) * rows + rs.start, ROWS), ROWS), :])

        @pl.when(jnp.logical_and(lo, step < steps - 2))
        def _():
            b_copy(group, step + 2).wait_send()

    def backward_cell(group, step, slot):
        for block in range(hidden // COLS):
            cs = cols_of(block)
            sums = [None] * 4
            for r in range(0, rows, B_ROWS):
                rs = slice(r, r + B_ROWS)
                at = pl.ds(pl.multiple_of(step * rows + r, B_ROWS), B_ROWS)
                f = [gates[slot, rs, part * hidden + cs.start:part * hidden + cs.stop] for part in range(6)]
                d_h = dhs[group, rs, cs] + dout[group, at, cs].astype(F32)
                d_cell = d_h * f[4] + dcs[group, rs, cs]
                dcs[group, rs, cs] = d_cell * f[5]
                for q, value in enumerate((d_cell * f[0], d_cell * f[1], d_cell * f[2], d_h * f[3])):
                    low = value.astype(BF16)
                    now[q, rs, cs] = low
                    dz[group][q, at, cs] = low
                    part = jnp.sum(value.reshape(B_ROWS // 8, 8, COLS), axis=0)
                    sums[q] = part if sums[q] is None else sums[q] + part
            for q in range(4):
                g_bias[q, :, cs] += sums[q]

    def through(weights, store):
        held = [None]
        n_blocks = hidden // COLS

        def piece(block, q):
            part = mm(now[q, :, cols_of(block)], weights[q, cols_of(block), :])
            held[0] = part if held[0] is None else held[0] + part
            if block == n_blocks - 1 and q == 3:
                store(held[0])

        return [functools.partial(piece, block, q) for block in range(n_blocks) for q in range(4)]

    def backward_state(group):
        def store(value):
            dhs[group] = value

        return through(wrec_t, store)

    def backward_mm(group, step):
        def store(value):
            ring_d[group, lax.rem(step, 2)] = value.astype(BF16)

        for piece in through(win_t, store):
            piece()

    def backward_send(group, step):
        @pl.when(lo)
        def _():
            b_copy(group, step).start()

    def weight_tile(group, tick):
        q, m = lax.div(tick, 4), lax.rem(tick, 4)
        across = pl.ds(pl.multiple_of(m * (hidden // 4), hidden // 4), hidden // 4)

        def piece(which):
            lhs = seq[group, :, across] if which == 0 else hist[group, 0:steps * rows, across]
            gates[tick, :, which * hidden:(which + 1) * hidden] = mm_t(lhs, dz[group][q])

        return [functools.partial(piece, which) for which in range(2)]

    def tile_copy(tick, which):
        q, m = lax.div(tick, 4), lax.rem(tick, 4)
        part = hidden // 4
        return pltpu.make_async_copy(
            gates.at[tick, :, pl.ds(which * hidden, hidden)],
            partial_ref.at[which, pl.ds(pl.multiple_of(m * part, part), part), pl.ds(pl.multiple_of(q * hidden, hidden), hidden)],
            tile_sem.at[which, tick])

    def phase_1(step, _):
        interleave(forward_old(0, step), [])
        forward_wait(0, step)
        forward_new(0, step, dhs.at[1])
        forward_send(0, step)
        return 0

    lax.fori_loop(0, steps, phase_1, 0)

    @pl.when(first)
    def _():
        land(inputs_ref, 1).wait()
        time_major(1, seq)

    again = load(c0_ref.at[pl.ds(rows, rows), :], dhs.at[1], 8)
    again.start()

    def phase_2(step, _):
        new = recompute_mm(0, step)
        recompute_cell(0, step, step, dhs.at[0], new, 0)
        interleave(forward_old(1, step), [])
        recompute_cell(0, step, step, dhs.at[0], new, 1)
        forward_wait(1, step)
        forward_new(1, step, dcs.at[1])
        forward_send(1, step)
        return 0

    lax.fori_loop(0, steps, phase_2, 0)
    again.wait()

    @pl.when(jnp.logical_not(early))
    def _():
        set_up()

    def backward(group, step, slot):
        backward_wait(group, step)
        backward_cell(group, step, slot)
        backward_mm(group, step)
        backward_send(group, step)

    dhs[0] = jnp.zeros((rows, hidden), F32)
    dcs[0] = jnp.zeros((rows, hidden), F32)

    def phase_3(tick, _):
        step = steps - 1 - tick
        backward(0, step, step)
        new = recompute_mm(1, tick)
        recompute_cell(1, tick, steps - tick, dhs.at[1], new, 0)
        interleave(backward_state(0), [])
        recompute_cell(1, tick, steps - tick, dhs.at[1], new, 1)
        return 0

    lax.fori_loop(0, steps, phase_3, 0)
    dhs[1] = jnp.zeros((rows, hidden), F32)
    dcs[1] = jnp.zeros((rows, hidden), F32)

    def tile_start(tick):
        for which in range(2):
            tile_copy(tick, which).start()

    def phase_4(tick, _):
        step = steps - 1 - tick
        backward(1, step, steps - step)

        @pl.when(early)
        def _():
            interleave(backward_state(1), [])

        @pl.when(jnp.logical_not(early))
        def _():
            @pl.when(tick > 0)
            def _():
                tile_start(tick - 1)

            interleave(backward_state(1), [])
            interleave(weight_tile(0, tick), [])

        return 0

    lax.fori_loop(0, steps, phase_4, 0)

    @pl.when(top)
    def _():
        total = jnp.sum(loss_acc[...]) * (0.5 * scale)
        loss_buf[...] = jnp.full(loss_buf.shape, total, F32)
        loss_copy().start()

    @pl.when(hi)
    def _():
        loss_copy().wait_recv()

        @pl.when(lo)
        def _():
            loss_copy().start()

    def late_tile(tick, _):
        interleave(weight_tile(0, tick), [])

        @pl.when(tick > 0)
        def _():
            tile_start(tick - 1)

        return 0

    @pl.when(early)
    def _():
        lax.fori_loop(0, steps, late_tile, 0)

    tile_start(steps - 1)

    def tile_wait(tick, _):
        for which in range(2):
            tile_copy(tick, which).wait()
        return 0

    lax.fori_loop(0, steps, tile_wait, 0)

    @pl.when(hi)
    def _():
        for group in range(2):
            for step in (steps - 2, steps - 1):
                f_copy(group, step).wait_send()

    @pl.when(lo)
    def _():
        for group in range(2):
            for step in (1, 0):
                b_copy(group, step).wait_send()
        loss_copy().wait_send()


def finish_kernel(steps, rows, hidden, partial_ref, dz, hist, seq, dhs, dcs, g_bias, loss_buf,
                  loss_ref, g_in_ref, g_rec_ref, g_bias_ref, dh0_ref, dc0_ref, total, in_sem, out_sem, state_sem):
    def take(q, which):
        cols = pl.ds(pl.multiple_of(q * hidden, hidden), hidden)
        return pltpu.make_async_copy(partial_ref.at[which, :, cols], total.at[q, which], in_sem.at[q, which])

    def put(q, which):
        cols = pl.ds(pl.multiple_of(q * hidden, hidden), hidden)
        return pltpu.make_async_copy(total.at[q, which], (g_in_ref, g_rec_ref)[which].at[:, cols], out_sem.at[q, which])

    for q in range(4):
        for which in range(2):
            take(q, which).start()
    states = []
    for group in range(2):
        at = pl.ds(group * rows, rows)
        states.append(pltpu.make_async_copy(dhs.at[group], dh0_ref.at[at, :], state_sem.at[group]))
        states.append(pltpu.make_async_copy(dcs.at[group], dc0_ref.at[at, :], state_sem.at[2 + group]))
    for copy in states:
        copy.start()
    loss_ref[0] = loss_buf[0, 0]
    for q in range(4):
        g_bias_ref[:, q * hidden:(q + 1) * hidden] = jnp.sum(g_bias[q], axis=0, keepdims=True)

    def gate(q, _):
        new = [mm_t(lhs, dz[q]) for lhs in (seq[1], hist[1, 0:steps * rows, :])]
        for which in range(2):
            take(q, which).wait()
        for which in range(2):
            total[q, which] = total[q, which] + new[which]
            put(q, which).start()
        return 0

    lax.fori_loop(0, 4, gate, 0)
    for copy in states:
        copy.wait()
    for q in range(4):
        for which in range(2):
            put(q, which).wait()


def solution(mesh):
    last = mesh.shape['stage'] - 1

    def local(inputs, targets, lengths, w_in, w_rec, bias, h_init, c_init):
        batch, steps, hidden = inputs.shape
        rows = batch // 2
        wide = 4 * hidden
        any_spec = pl.BlockSpec(memory_space=pl.ANY)
        vmem_spec = pl.BlockSpec(memory_space=pltpu.VMEM)
        dma = pltpu.SemaphoreType.DMA
        held = pl.pallas_call(
            functools.partial(kernel, last, steps, rows, hidden),
            out_shape=(
                jax.ShapeDtypeStruct((8, hidden, wide), F32),
                pltpu.VMEM((4, steps * rows, hidden), BF16),
                pltpu.VMEM((2, (steps + 1) * rows, hidden), BF16),
                pltpu.VMEM((2, steps * rows, hidden), BF16),
                pltpu.VMEM((2, rows, hidden), F32),
                pltpu.VMEM((2, rows, hidden), F32),
                pltpu.VMEM((4, 8, hidden), F32),
                pltpu.VMEM((8, 128), F32)),
            in_specs=[any_spec, any_spec, vmem_spec, any_spec, any_spec, vmem_spec, any_spec, any_spec],
            out_specs=(any_spec,) + (vmem_spec,) * 7,
            scratch_shapes=[
                pltpu.VMEM((steps + 1, rows, 6 * hidden), F32),
                pltpu.VMEM((4, steps * rows, hidden), BF16),
                pltpu.VMEM((4, rows, hidden), BF16),
                pltpu.VMEM((2, steps * rows, hidden), BF16),
                pltpu.VMEM((4, hidden, hidden), BF16),
                pltpu.VMEM((4, hidden, hidden), BF16),
                pltpu.VMEM((2, 2, rows, hidden), BF16),
                pltpu.VMEM((2, 2, rows, hidden), BF16),
                pltpu.VMEM((rows, 4 * hidden), F32),
                pltpu.VMEM((2, rows, 128), F32),
                pltpu.VMEM((8, hidden), F32),
                pltpu.VMEM((8, 128), F32),
                dma((2, steps)), dma((2, 2)), dma((2, steps)), dma((2, 2)), dma, dma, dma((15,)), dma((2, steps))],
            compiler_params=pltpu.CompilerParams(
                collective_id=0, has_side_effects=True, vmem_limit_bytes=HELD_LIMIT),
        )(inputs.reshape(batch * steps, hidden), targets.reshape(batch * steps, hidden), lengths.reshape(2, rows),
          w_in[0], w_rec[0], bias, h_init[0], c_init[0])
        loss, g_in, g_rec, g_bias, dh0, dc0 = pl.pallas_call(
            functools.partial(finish_kernel, steps, rows, hidden),
            out_shape=(
                jax.ShapeDtypeStruct((1,), F32),
                jax.ShapeDtypeStruct((hidden, wide), F32),
                jax.ShapeDtypeStruct((hidden, wide), F32),
                jax.ShapeDtypeStruct((1, wide), F32),
                jax.ShapeDtypeStruct((batch, hidden), F32),
                jax.ShapeDtypeStruct((batch, hidden), F32)),
            in_specs=[pl.BlockSpec(memory_space=pltpu.HBM)] + [vmem_spec] * 7,
            out_specs=(pl.BlockSpec(memory_space=pltpu.SMEM), any_spec, any_spec, vmem_spec, any_spec, any_spec),
            scratch_shapes=[pltpu.VMEM((4, 2, hidden, hidden), F32), dma((4, 2)), dma((4, 2)), dma((4,))],
            compiler_params=pltpu.CompilerParams(vmem_limit_bytes=FINISH_LIMIT),
        )(*held)
        return loss, g_in[None], g_rec[None], g_bias, dh0[None], dc0[None]

    layer_spec = P(('data', 'stage'))
    return jax.shard_map(
        local, mesh=mesh,
        in_specs=(P('data'), P('data'), P('data'), P('stage'), P('stage'), P('stage'), P('stage', 'data'), P('stage', 'data')),
        out_specs=(P('data'), layer_spec, layer_spec, layer_spec, P('stage', 'data'), P('stage', 'data')),
        check_vma=False)
```

```python
import functools

import jax
import jax.numpy as jnp
from jax import lax
from jax.experimental import pallas as pl
from jax.experimental.pallas import tpu as pltpu
from jax.sharding import PartitionSpec as P

F32 = jnp.float32
BF16 = jnp.bfloat16
COLS = 256
ROWS = 32
B_ROWS = 16
ORDER = (0, 2, 1, 3)
HELD_LIMIT = 48_200_000
FINISH_LIMIT = 16_000_000


def mm(lhs, rhs):
    return jnp.dot(lhs, rhs, preferred_element_type=F32)


def mm_t(lhs, rhs):
    return lax.dot_general(lhs, rhs, (((0,), (0,)), ((), ())), preferred_element_type=F32)


def sigmoid(value):
    return 0.5 * jnp.tanh(0.5 * value) + 0.5


def interleave(main, side):
    done = 0
    for idx, piece in enumerate(main):
        upto = (idx + 1) * len(side) // len(main)
        for other in side[done:upto]:
            other()
        done = upto
        piece()


def kernel(last, steps, rows, hidden,
           inputs_ref, targets_ref, lens_hbm, w_in_ref, w_rec_ref, bias_hbm, h0_ref, c0_ref,
           partial_ref, dz_1, hist, seq, dhs, dcs, g_bias, loss_buf, last_tile,
           gates, dz_0, now, dout, win_t, wrec_t, ring_h, ring_d, work, lens, loss_acc, fence, bias_all, lens_all,
           f_recv, f_send, b_recv, b_send, loss_recv, loss_send, local_sem, tile_sem):
    stage = lax.axis_index('stage')
    bias_ref = bias_all.at[pl.ds(0, 1)]
    lens_ref = lens_all.at[pl.ds(0, 2)]
    lo, hi = stage > 0, stage < last
    first, top = stage == 0, stage == last
    dz = (dz_0, dz_1)
    win, wrec = dz_1.at[:, pl.ds(0, hidden), :], dz_1.at[:, pl.ds(hidden, hidden), :]
    batch = 2 * rows
    scale = 1.0 / (batch * steps)

    def at_step(step):
        return pl.ds(pl.multiple_of(step * rows, rows), rows)

    def f_copy(group, step):
        slot = lax.rem(step, 2)
        return pltpu.make_async_remote_copy(
            src_ref=ring_h.at[group, slot], dst_ref=seq.at[group, at_step(step), :],
            send_sem=f_send.at[group, slot], recv_sem=f_recv.at[group, step],
            device_id={'stage': stage + 1}, device_id_type=pl.DeviceIdType.MESH)

    def b_copy(group, step):
        slot = lax.rem(step, 2)
        return pltpu.make_async_remote_copy(
            src_ref=ring_d.at[group, slot], dst_ref=dout.at[group, at_step(step), :],
            send_sem=b_send.at[group, slot], recv_sem=b_recv.at[group, step],
            device_id={'stage': stage - 1}, device_id_type=pl.DeviceIdType.MESH)

    def loss_copy():
        return pltpu.make_async_remote_copy(
            src_ref=loss_buf, dst_ref=loss_buf, send_sem=loss_send, recv_sem=loss_recv,
            device_id={'stage': stage - 1}, device_id_type=pl.DeviceIdType.MESH)

    def load(src, dst, sem):
        return pltpu.make_async_copy(src, dst, local_sem.at[sem])

    smalls = [load(lens_hbm, lens_ref, 15), load(bias_hbm, bias_ref, 16)]
    for copy in smalls:
        copy.start()
    loads = []
    for q in range(4):
        cols = pl.ds(q * hidden, hidden)
        loads.append(load(w_rec_ref.at[:, cols], wrec.at[q], 4 + q))
    for q in range(4):
        cols = pl.ds(q * hidden, hidden)
        loads.append(load(w_in_ref.at[:, cols], win.at[q], 0 + q))
    loads.append(load(c0_ref.at[pl.ds(0, rows), :], dhs.at[1], 8))
    loads.append(load(c0_ref.at[pl.ds(rows, rows), :], dcs.at[1], 9))
    loads.append(load(c0_ref.at[pl.ds(0, rows), :], dhs.at[0], 10))
    loads.append(load(h0_ref.at[pl.ds(0, rows), :], gates.at[0, :, pl.ds(0, hidden)], 11))
    loads.append(load(h0_ref.at[pl.ds(rows, rows), :], gates.at[1, :, pl.ds(0, hidden)], 12))

    def land(src, group):
        return load(src.at[pl.ds(group * rows * steps, rows * steps), :],
                    dz_0.at[group], 13 + group)

    @pl.when(first)
    def _():
        land(inputs_ref, 0).start()

    for copy in loads:
        copy.start()

    @pl.when(first)
    def _():
        land(inputs_ref, 1).start()

    @pl.when(top)
    def _():
        for group in range(2):
            land(targets_ref, group).start()

    barrier = pltpu.get_barrier_semaphore()

    @pl.when(lo)
    def _():
        pl.semaphore_signal(barrier, inc=1, device_id={'stage': stage - 1}, device_id_type=pl.DeviceIdType.MESH)

    @pl.when(hi)
    def _():
        pl.semaphore_signal(barrier, inc=1, device_id={'stage': stage + 1}, device_id_type=pl.DeviceIdType.MESH)

    for copy in smalls:
        copy.wait()
    for group in range(2):
        row = lens_ref[group:group + 1, :].astype(F32)
        lens[group] = jnp.broadcast_to(row, (128, rows)).T

    loss_acc[...] = jnp.zeros_like(loss_acc)
    g_bias[...] = jnp.zeros_like(g_bias)

    def time_major(group, dst):
        size = 16 * steps
        out_row = lax.broadcasted_iota(jnp.int32, (size, size), 0)
        in_row = lax.broadcasted_iota(jnp.int32, (size, size), 1)
        step_of, row_of = lax.div(out_row, 16), lax.rem(out_row, 16)
        permute = (in_row == row_of * steps + step_of).astype(F32).astype(BF16)

        def blocks(trip, _):
            for idx in (trip * 2, trip * 2 + 1):
                piece = dz_0[group, pl.ds(pl.multiple_of(idx * size, size), size), :]
                moved = mm(permute, piece).astype(BF16)
                for step in range(steps):
                    dst[group, pl.ds(pl.multiple_of(step * rows + idx * 16, 16), 16), :] = moved[step * 16:(step + 1) * 16]
            return 0

        lax.fori_loop(0, rows // 32, blocks, 0)

    def set_up():
        def turn(q, _):
            win_t[q] = win[q].T
            wrec_t[q] = wrec[q].T
            return 0

        lax.fori_loop(0, 4, turn, 0)

    @pl.when(first)
    def _():
        land(inputs_ref, 0).wait()
        time_major(0, seq)

    for copy in loads:
        copy.wait()
    for group in range(2):
        h_start = gates[group, :, 0:hidden].astype(BF16)
        hist[group, 0:rows, :] = h_start
        ring_h[group, 1] = h_start

    @pl.when(top)
    def _():
        for group in range(2):
            land(targets_ref, group).wait()
            time_major(group, dout)

    early = stage >= (last + 1) // 2

    @pl.when(early)
    def _():
        set_up()

    def cols_of(block):
        return slice(block * COLS, (block + 1) * COLS)

    def bias_of(q, block):
        return bias_ref[:, q * hidden + block * COLS:q * hidden + (block + 1) * COLS]

    def cell(group, step, z, c_ref, rs, cs, slot=None):
        in_gate, cand = sigmoid(z[0]), jnp.tanh(z[2])
        forget = sigmoid(z[1])
        new, old = in_gate * cand, forget * c_ref[rs, cs]
        c_new = old + new
        c_ref[rs, cs] = c_new
        tanh_c = jnp.tanh(c_new)
        out_gate = sigmoid(z[3])
        out = out_gate * tanh_c
        if slot is not None:
            values = (new * (1.0 - in_gate), old * (1.0 - forget), in_gate - new * cand, out * (1.0 - out_gate),
                      out_gate - out * tanh_c, forget)
            for part, value in enumerate(values):
                gates[slot, rs, part * hidden + cs.start:part * hidden + cs.stop] = value
        live = jnp.tile(lens[group, rs, :] > step.astype(F32), (1, COLS // 128))
        return jnp.where(live, out, 0.0).astype(BF16)

    def row_blocks():
        return [slice(r, r + ROWS) for r in range(0, rows, ROWS)]

    def forward_old(group, step):
        def piece(q):
            h = ring_h[group, 1 - lax.rem(step, 2)]
            at = slice(q * hidden, (q + 1) * hidden)
            work[:, at] = mm(h, wrec[q]) + bias_ref[:, at]

        return [functools.partial(piece, q) for q in ORDER]

    def forward_wait(group, step):
        @pl.when(jnp.logical_and(hi, step >= 2))
        def _():
            f_copy(group, step - 2).wait_send()

        @pl.when(lo)
        def _():
            f_copy(group, step).wait_recv()
            fence[...] = jnp.zeros_like(fence)

    def forward_new(group, step, c_ref):
        slot = lax.rem(step, 2)
        x = seq[group, at_step(step), :]
        n_blocks = hidden // COLS
        order = [(q, block) for block in range(n_blocks) for q in (0, 1, 2)] + [(3, block) for block in range(n_blocks)]
        new = {(q, block): mm(x, win[q, :, cols_of(block)]) for q, block in order}
        bent = {}

        def z(q, block, rs):
            return new[q, block][rs] + work[rs, q * hidden + block * COLS:q * hidden + (block + 1) * COLS]

        for block in range(n_blocks):
            cs = cols_of(block)
            for rs in row_blocks():
                in_gate, cand, forget = sigmoid(z(0, block, rs)), jnp.tanh(z(2, block, rs)), sigmoid(z(1, block, rs))
                c_new = forget * c_ref[rs, cs] + in_gate * cand
                c_ref[rs, cs] = c_new
                live = jnp.tile(lens[group, rs, :] > step.astype(F32), (1, COLS // 128))
                bent[block, rs.start] = jnp.where(live, 0.5 * jnp.tanh(c_new), 0.0)
        for block in range(n_blocks):
            for rs in row_blocks():
                out = (jnp.tanh(0.5 * z(3, block, rs)) + 1.0) * bent[block, rs.start]
                ring_h[group, slot, rs, cols_of(block)] = out.astype(BF16)

    def forward_send(group, step):
        @pl.when(hi)
        def _():
            f_copy(group, step).start()

        if group == 0:
            @pl.when(top)
            def _():
                output_error(group, step, lambda rs: ring_h[group, lax.rem(step, 2), rs, :])

    def output_error(group, step, made):
        for rs in row_blocks():
            at = pl.ds(pl.multiple_of(step * rows + rs.start, ROWS), ROWS)
            live = jnp.tile(lens[group, rs, :] > step.astype(F32), (1, hidden // 128))
            error = jnp.where(live, made(rs).astype(F32) - dout[group, at, :].astype(F32), 0.0)
            loss_acc[...] += jnp.sum((error * error).reshape(ROWS // 8, 8, hidden), axis=0)
            dout[group, at, :] = (error * scale).astype(BF16)

    def recompute_mm(group, step):
        x = seq[group, at_step(step), :]
        h = hist[group, at_step(step), :]
        return [{q: mm(x, win[q, :, cols_of(block)]) + mm(h, wrec[q, :, cols_of(block)]) for q in ORDER}
                for block in range(hidden // COLS)]

    def recompute_cell(group, step, slot, c_ref, new, block):
        cs = cols_of(block)
        for rs in row_blocks():
            z = [new[block][q][rs] + bias_of(q, block) for q in range(4)]
            at = pl.ds(pl.multiple_of((step + 1) * rows + rs.start, ROWS), ROWS)
            hist[group, at, cs] = cell(group, step, z, c_ref, rs, cs, slot)

    def backward_wait(group, step):
        @pl.when(jnp.logical_and(lo, step < steps - 2))
        def _():
            b_copy(group, step + 2).wait_send()

        @pl.when(hi)
        def _():
            b_copy(group, step).wait_recv()
            fence[...] = jnp.zeros_like(fence)

        if group == 1:
            @pl.when(jnp.logical_and(top, step >= steps // 2))
            def _():
                for later in (2 * step - steps + 1, 2 * step - steps):
                    output_error(group, later, lambda rs, later=later: hist[
                        group, pl.ds(pl.multiple_of((later + 1) * rows + rs.start, ROWS), ROWS), :])

    def backward_cell(group, step, slot):
        def part(number, rs, cs):
            return gates[slot, rs, number * hidden + cs.start:number * hidden + cs.stop]

        def keep(q, value, rs, cs, sums):
            low = value.astype(BF16)
            now[q, rs, cs] = low
            dz[group][q, pl.ds(pl.multiple_of(step * rows + rs.start, B_ROWS), B_ROWS), cs] = low
            folded = jnp.sum(value.reshape(B_ROWS // 8, 8, COLS), axis=0)
            sums[q] = folded if sums[q] is None else sums[q] + folded

        blocks = [cols_of(block) for block in range(hidden // COLS)]
        pieces = [slice(r, r + B_ROWS) for r in range(0, rows, B_ROWS)]
        for cs in blocks:
            sums = [None] * 4
            for rs in pieces:
                at = pl.ds(pl.multiple_of(step * rows + rs.start, B_ROWS), B_ROWS)
                d_h = dhs[group, rs, cs] + dout[group, at, cs].astype(F32)
                dhs[group, rs, cs] = d_h
                keep(3, d_h * part(3, rs, cs), rs, cs, sums)
            g_bias[3, :, cs] += sums[3]
        for cs in blocks:
            sums = [None] * 4
            for rs in pieces:
                d_cell = dhs[group, rs, cs] * part(4, rs, cs) + dcs[group, rs, cs]
                dcs[group, rs, cs] = d_cell * part(5, rs, cs)
                for q in range(3):
                    keep(q, d_cell * part(q, rs, cs), rs, cs, sums)
            for q in range(3):
                g_bias[q, :, cs] += sums[q]

    def through(weights, store):
        held = [None]
        n_blocks = hidden // COLS

        order = [(block, 3) for block in range(n_blocks)] + [(block, q) for block in range(n_blocks) for q in range(3)]

        def piece(block, q):
            part = mm(now[q, :, cols_of(block)], weights[q, cols_of(block), :])
            held[0] = part if held[0] is None else held[0] + part
            if (block, q) == order[-1]:
                store(held[0])

        return [functools.partial(piece, block, q) for block, q in order]

    def backward_state(group):
        def store(value):
            dhs[group] = value

        return through(wrec_t, store)

    def backward_mm(group, step):
        def store(value):
            ring_d[group, lax.rem(step, 2)] = value.astype(BF16)

        for piece in through(win_t, store):
            piece()

    def backward_send(group, step):
        @pl.when(lo)
        def _():
            b_copy(group, step).start()

    def weight_tile(group, tick):
        q, m = lax.div(tick, 4), lax.rem(tick, 4)
        across = pl.ds(pl.multiple_of(m * (hidden // 4), hidden // 4), hidden // 4)

        def piece(which):
            lhs = seq[group, :, across] if which == 0 else hist[group, 0:steps * rows, across]
            gates[tick, :, which * hidden:(which + 1) * hidden] = mm_t(lhs, dz[group][q])

        return [functools.partial(piece, which) for which in range(2)]

    def tile_copy(tick, which):
        q, m = lax.div(tick, 4), lax.rem(tick, 4)
        part = hidden // 4
        return pltpu.make_async_copy(
            gates.at[tick, :, pl.ds(which * hidden, hidden)],
            partial_ref.at[which, pl.ds(pl.multiple_of(m * part, part), part), pl.ds(pl.multiple_of(q * hidden, hidden), hidden)],
            tile_sem.at[which, tick])

    def phase_1(step, _):
        interleave(forward_old(0, step), [])
        forward_wait(0, step)
        forward_new(0, step, dhs.at[1])
        forward_send(0, step)
        return 0

    @pl.when(jnp.logical_and(lo, hi))
    def _():
        pl.semaphore_wait(barrier, 2)

    @pl.when(jnp.logical_or(first, top))
    def _():
        pl.semaphore_wait(barrier, 1)

    lax.fori_loop(0, steps, phase_1, 0)

    @pl.when(first)
    def _():
        land(inputs_ref, 1).wait()
        time_major(1, seq)

    again = load(c0_ref.at[pl.ds(rows, rows), :], dhs.at[1], 8)
    again.start()

    def phase_2(step, _):
        new = recompute_mm(0, step)
        recompute_cell(0, step, step, dhs.at[0], new, 0)
        interleave(forward_old(1, step), [])
        recompute_cell(0, step, step, dhs.at[0], new, 1)
        forward_wait(1, step)
        forward_new(1, step, dcs.at[1])
        forward_send(1, step)
        return 0

    lax.fori_loop(0, steps, phase_2, 0)
    again.wait()

    @pl.when(jnp.logical_not(early))
    def _():
        set_up()

    def backward(group, step, slot):
        backward_wait(group, step)
        backward_cell(group, step, slot)
        backward_mm(group, step)
        backward_send(group, step)

    dhs[0] = jnp.zeros((rows, hidden), F32)
    dcs[0] = jnp.zeros((rows, hidden), F32)

    def phase_3(tick, _):
        step = steps - 1 - tick
        backward(0, step, step)
        new = recompute_mm(1, tick)
        recompute_cell(1, tick, steps - tick, dhs.at[1], new, 0)
        interleave(backward_state(0), [])
        recompute_cell(1, tick, steps - tick, dhs.at[1], new, 1)
        return 0

    lax.fori_loop(0, steps, phase_3, 0)
    dhs[1] = jnp.zeros((rows, hidden), F32)
    dcs[1] = jnp.zeros((rows, hidden), F32)

    def tile_copies(tick):
        @pl.when(tick > 0)
        def _():
            for which in range(2):
                tile_copy(tick - 1, which).start()

        @pl.when(tick > 1)
        def _():
            for which in range(2):
                tile_copy(tick - 2, which).wait()

    def loss_on():
        @pl.when(top)
        def _():
            total = jnp.sum(loss_acc[...]) * (0.5 * scale)
            loss_buf[...] = jnp.full(loss_buf.shape, total, F32)

        @pl.when(hi)
        def _():
            loss_copy().wait_recv()

        @pl.when(lo)
        def _():
            loss_copy().start()

    def phase_4(tick, _):
        step = steps - 1 - tick
        backward(1, step, steps - step)

        @pl.when(tick == steps - 4)
        def _():
            loss_on()

        @pl.when(early)
        def _():
            interleave(backward_state(1), [])

        @pl.when(jnp.logical_not(early))
        def _():
            tile_copies(tick)
            interleave(backward_state(1), [])
            interleave(weight_tile(0, tick), [])

        return 0

    lax.fori_loop(0, steps, phase_4, 0)

    def late_tile(tick, _):
        tile_copies(tick)
        interleave(weight_tile(0, tick), [])
        return 0

    @pl.when(early)
    def _():
        lax.fori_loop(0, steps, late_tile, 0)

    for which in range(2):
        last_tile[which] = gates[steps - 1, :, which * hidden:(which + 1) * hidden]
    for which in range(2):
        tile_copy(steps - 2, which).wait()

    @pl.when(hi)
    def _():
        for group in range(2):
            for step in (steps - 2, steps - 1):
                f_copy(group, step).wait_send()

    @pl.when(lo)
    def _():
        for group in range(2):
            for step in (1, 0):
                b_copy(group, step).wait_send()
        loss_copy().wait_send()


def finish_kernel(steps, rows, hidden, partial_ref, dz, hist, seq, dhs, dcs, g_bias, loss_buf, last_tile,
                  loss_ref, g_in_ref, g_rec_ref, g_bias_ref, dh0_ref, dc0_ref, total, in_sem, out_sem, state_sem):
    part = hidden // 4

    def take(q, which, piece):
        cols = pl.ds(pl.multiple_of(q * hidden, hidden), hidden)
        at = pl.ds(0, 3 * part) if piece == 0 else pl.ds(3 * part, part)
        return pltpu.make_async_copy(partial_ref.at[which, at, cols], total.at[q, which, at, :], in_sem.at[q, which, piece])

    def put(q, which):
        cols = pl.ds(pl.multiple_of(q * hidden, hidden), hidden)
        return pltpu.make_async_copy(total.at[q, which], (g_in_ref, g_rec_ref)[which].at[:, cols], out_sem.at[q, which])

    for q in range(4):
        for which in range(2):
            take(q, which, 0).start()
            if q < 3:
                take(q, which, 1).start()
    states = []
    for group in range(2):
        at = pl.ds(group * rows, rows)
        states.append(pltpu.make_async_copy(dhs.at[group], dh0_ref.at[at, :], state_sem.at[group]))
        states.append(pltpu.make_async_copy(dcs.at[group], dc0_ref.at[at, :], state_sem.at[2 + group]))
    for copy in states:
        copy.start()
    loss_ref[0] = loss_buf[0, 0]
    for which in range(2):
        total[3, which, 3 * part:4 * part, :] = last_tile[which]
    for q in range(4):
        g_bias_ref[:, q * hidden:(q + 1) * hidden] = jnp.sum(g_bias[q], axis=0, keepdims=True)

    def gate(q, _):
        new = [mm_t(lhs, dz[q]) for lhs in (seq[1], hist[1, 0:steps * rows, :])]
        for which in range(2):
            take(q, which, 0).wait()

        @pl.when(q < 3)
        def _():
            for which in range(2):
                take(q, which, 1).wait()

        for which in range(2):
            total[q, which] = total[q, which] + new[which]
            put(q, which).start()
        return 0

    lax.fori_loop(0, 4, gate, 0)
    for copy in states:
        copy.wait()
    for q in range(4):
        for which in range(2):
            put(q, which).wait()


def solution(mesh):
    last = mesh.shape['stage'] - 1

    def local(inputs, targets, lengths, w_in, w_rec, bias, h_init, c_init):
        batch, steps, hidden = inputs.shape
        rows = batch // 2
        wide = 4 * hidden
        any_spec = pl.BlockSpec(memory_space=pl.ANY)
        vmem_spec = pl.BlockSpec(memory_space=pltpu.VMEM)
        dma = pltpu.SemaphoreType.DMA
        held = pl.pallas_call(
            functools.partial(kernel, last, steps, rows, hidden),
            out_shape=(
                jax.ShapeDtypeStruct((8, hidden, wide), F32),
                pltpu.VMEM((4, steps * rows, hidden), BF16),
                pltpu.VMEM((2, (steps + 1) * rows, hidden), BF16),
                pltpu.VMEM((2, steps * rows, hidden), BF16),
                pltpu.VMEM((2, rows, hidden), F32),
                pltpu.VMEM((2, rows, hidden), F32),
                pltpu.VMEM((4, 8, hidden), F32),
                pltpu.VMEM((8, 128), F32),
                pltpu.VMEM((2, hidden // 4, hidden), F32)),
            in_specs=[any_spec] * 8,
            out_specs=(any_spec,) + (vmem_spec,) * 8,
            scratch_shapes=[
                pltpu.VMEM((steps + 1, rows, 6 * hidden), F32),
                pltpu.VMEM((4, steps * rows, hidden), BF16),
                pltpu.VMEM((4, rows, hidden), BF16),
                pltpu.VMEM((2, steps * rows, hidden), BF16),
                pltpu.VMEM((4, hidden, hidden), BF16),
                pltpu.VMEM((4, hidden, hidden), BF16),
                pltpu.VMEM((2, 2, rows, hidden), BF16),
                pltpu.VMEM((2, 2, rows, hidden), BF16),
                pltpu.VMEM((rows, 4 * hidden), F32),
                pltpu.VMEM((2, rows, 128), F32),
                pltpu.VMEM((8, hidden), F32),
                pltpu.VMEM((32, 128), F32),
                pltpu.VMEM((8, wide), F32),
                pltpu.VMEM((32, 128), jnp.int32),
                dma((2, steps)), dma((2, 2)), dma((2, steps)), dma((2, 2)), dma, dma, dma((17,)), dma((2, steps))],
            compiler_params=pltpu.CompilerParams(
                collective_id=0, has_side_effects=True, vmem_limit_bytes=HELD_LIMIT),
        )(inputs.reshape(batch * steps, hidden), targets.reshape(batch * steps, hidden), lengths.reshape(2, rows),
          w_in[0], w_rec[0], bias, h_init[0], c_init[0])
        loss, g_in, g_rec, g_bias, dh0, dc0 = pl.pallas_call(
            functools.partial(finish_kernel, steps, rows, hidden),
            out_shape=(
                jax.ShapeDtypeStruct((1,), F32),
                jax.ShapeDtypeStruct((hidden, wide), F32),
                jax.ShapeDtypeStruct((hidden, wide), F32),
                jax.ShapeDtypeStruct((1, wide), F32),
                jax.ShapeDtypeStruct((batch, hidden), F32),
                jax.ShapeDtypeStruct((batch, hidden), F32)),
            in_specs=[pl.BlockSpec(memory_space=pltpu.HBM)] + [vmem_spec] * 8,
            out_specs=(pl.BlockSpec(memory_space=pltpu.SMEM), any_spec, any_spec, vmem_spec, any_spec, any_spec),
            scratch_shapes=[pltpu.VMEM((4, 2, hidden, hidden), F32), dma((4, 2, 2)), dma((4, 2)), dma((4,))],
            compiler_params=pltpu.CompilerParams(vmem_limit_bytes=FINISH_LIMIT),
        )(*held)
        return loss, g_in[None], g_rec[None], g_bias, dh0[None], dc0[None]

    layer_spec = P(('data', 'stage'))
    return jax.shard_map(
        local, mesh=mesh,
        in_specs=(P('data'), P('data'), P('data'), P('stage'), P('stage'), P('stage'), P('stage', 'data'), P('stage', 'data')),
        out_specs=(P('data'), layer_spec, layer_spec, layer_spec, P('stage', 'data'), P('stage', 'data')),
        check_vma=False)
```

```python
import functools

import jax
import jax.numpy as jnp
from jax import lax
from jax.experimental import pallas as pl
from jax.experimental.pallas import tpu as pltpu
from jax.sharding import PartitionSpec as P

F32 = jnp.float32
BF16 = jnp.bfloat16
COLS = 256
ROWS = 32
B_ROWS = 16
ORDER = (0, 2, 1, 3)
HELD_LIMIT = 48_200_000
FINISH_LIMIT = 16_000_000


def mm(lhs, rhs):
    return jnp.dot(lhs, rhs, preferred_element_type=F32)


def mm_t(lhs, rhs):
    return lax.dot_general(lhs, rhs, (((0,), (0,)), ((), ())), preferred_element_type=F32)


def sigmoid(value):
    return 0.5 * jnp.tanh(0.5 * value) + 0.5


def interleave(main, side):
    done = 0
    for idx, piece in enumerate(main):
        upto = (idx + 1) * len(side) // len(main)
        for other in side[done:upto]:
            other()
        done = upto
        piece()


def kernel(last, steps, rows, hidden,
           inputs_ref, targets_ref, lens_hbm, w_in_ref, w_rec_ref, bias_hbm, h0_ref, c0_ref,
           partial_ref, dz_1, hist, seq, dhs, dcs, g_bias, loss_buf, last_tile,
           gates, dz_0, now, dout, win_t, wrec_t, ring_h, ring_d, work, lens, loss_acc, fence, bias_all, lens_all,
           f_recv, f_send, b_recv, b_send, loss_recv, loss_send, local_sem, tile_sem):
    stage = lax.axis_index('stage')
    bias_ref = bias_all.at[pl.ds(0, 1)]
    lens_ref = lens_all.at[pl.ds(0, 2)]
    lo, hi = stage > 0, stage < last
    first, top = stage == 0, stage == last
    dz = (dz_0, dz_1)
    win, wrec = dz_1.at[:, pl.ds(0, hidden), :], dz_1.at[:, pl.ds(hidden, hidden), :]
    batch = 2 * rows
    scale = 1.0 / (batch * steps)

    def at_step(step):
        return pl.ds(pl.multiple_of(step * rows, rows), rows)

    def f_copy(group, step):
        slot = lax.rem(step, 2)
        return pltpu.make_async_remote_copy(
            src_ref=ring_h.at[group, slot], dst_ref=seq.at[group, at_step(step), :],
            send_sem=f_send.at[group, slot], recv_sem=f_recv.at[group, step],
            device_id={'stage': stage + 1}, device_id_type=pl.DeviceIdType.MESH)

    def b_copy(group, step):
        slot = lax.rem(step, 2)
        return pltpu.make_async_remote_copy(
            src_ref=ring_d.at[group, slot], dst_ref=dout.at[group, at_step(step), :],
            send_sem=b_send.at[group, slot], recv_sem=b_recv.at[group, step],
            device_id={'stage': stage - 1}, device_id_type=pl.DeviceIdType.MESH)

    def loss_copy():
        return pltpu.make_async_remote_copy(
            src_ref=loss_buf, dst_ref=loss_buf, send_sem=loss_send, recv_sem=loss_recv,
            device_id={'stage': stage - 1}, device_id_type=pl.DeviceIdType.MESH)

    def load(src, dst, sem):
        return pltpu.make_async_copy(src, dst, local_sem.at[sem])

    smalls = [load(lens_hbm, lens_ref, 15), load(bias_hbm, bias_ref, 16)]
    for copy in smalls:
        copy.start()
    loads = []
    for q in range(4):
        cols = pl.ds(q * hidden, hidden)
        loads.append(load(w_rec_ref.at[:, cols], wrec.at[q], 4 + q))
    for q in range(4):
        cols = pl.ds(q * hidden, hidden)
        loads.append(load(w_in_ref.at[:, cols], win.at[q], 0 + q))
    loads.append(load(c0_ref.at[pl.ds(0, rows), :], dhs.at[1], 8))
    loads.append(load(h0_ref.at[pl.ds(0, rows), :], gates.at[0, :, pl.ds(0, hidden)], 11))
    late_loads = [
        load(c0_ref.at[pl.ds(rows, rows), :], dcs.at[1], 9),
        load(c0_ref.at[pl.ds(0, rows), :], dhs.at[0], 10),
        load(h0_ref.at[pl.ds(rows, rows), :], gates.at[1, :, pl.ds(0, hidden)], 12)]

    def land(src, group):
        return load(src.at[pl.ds(group * rows * steps, rows * steps), :],
                    dz_0.at[group], 13 + group)

    @pl.when(first)
    def _():
        land(inputs_ref, 0).start()

    for copy in loads[8:] + loads[:8]:
        copy.start()

    @pl.when(top)
    def _():
        for group in range(2):
            land(targets_ref, group).start()

    barrier = pltpu.get_barrier_semaphore()

    @pl.when(lo)
    def _():
        pl.semaphore_signal(barrier, inc=1, device_id={'stage': stage - 1}, device_id_type=pl.DeviceIdType.MESH)

    @pl.when(hi)
    def _():
        pl.semaphore_signal(barrier, inc=1, device_id={'stage': stage + 1}, device_id_type=pl.DeviceIdType.MESH)

    for copy in smalls:
        copy.wait()
    for group in range(2):
        row = lens_ref[group:group + 1, :].astype(F32)
        lens[group] = jnp.broadcast_to(row, (128, rows)).T

    loss_acc[...] = jnp.zeros_like(loss_acc)
    g_bias[...] = jnp.zeros_like(g_bias)

    def time_major(group, dst):
        size = 16 * steps
        out_row = lax.broadcasted_iota(jnp.int32, (size, size), 0)
        in_row = lax.broadcasted_iota(jnp.int32, (size, size), 1)
        step_of, row_of = lax.div(out_row, 16), lax.rem(out_row, 16)
        permute = (in_row == row_of * steps + step_of).astype(F32).astype(BF16)

        def blocks(trip, _):
            for idx in [trip * 4 + sub for sub in range(4)]:
                piece = dz_0[group, pl.ds(pl.multiple_of(idx * size, size), size), :]
                moved = mm(permute, piece).astype(BF16)
                for step in range(steps):
                    dst[group, pl.ds(pl.multiple_of(step * rows + idx * 16, 16), 16), :] = moved[step * 16:(step + 1) * 16]
            return 0

        lax.fori_loop(0, rows // 64, blocks, 0)

    def set_up():
        def turn(q, _):
            win_t[q] = win[q].T
            wrec_t[q] = wrec[q].T
            return 0

        lax.fori_loop(0, 4, turn, 0)

    @pl.when(first)
    def _():
        land(inputs_ref, 0).wait()
        time_major(0, seq)

    for copy in loads[8:]:
        copy.wait()

    def first_state(group):
        h_start = gates[group, :, 0:hidden].astype(BF16)
        hist[group, 0:rows, :] = h_start
        ring_h[group, 1] = h_start

    first_state(0)

    @pl.when(top)
    def _():
        for group in range(2):
            land(targets_ref, group).wait()
            time_major(group, dout)

    for copy in loads[:8]:
        copy.wait()
    early = stage >= (last + 1) // 2

    @pl.when(early)
    def _():
        set_up()

    def cols_of(block):
        return slice(block * COLS, (block + 1) * COLS)

    def bias_of(q, block):
        return bias_ref[:, q * hidden + block * COLS:q * hidden + (block + 1) * COLS]

    def cell(group, step, z, c_ref, rs, cs, slot=None):
        in_gate, cand = sigmoid(z[0]), jnp.tanh(z[2])
        forget = sigmoid(z[1])
        new, old = in_gate * cand, forget * c_ref[rs, cs]
        c_new = old + new
        c_ref[rs, cs] = c_new
        tanh_c = jnp.tanh(c_new)
        out_gate = sigmoid(z[3])
        out = out_gate * tanh_c
        if slot is not None:
            values = (new * (1.0 - in_gate), old * (1.0 - forget), in_gate - new * cand, out * (1.0 - out_gate),
                      out_gate - out * tanh_c, forget)
            for part, value in enumerate(values):
                gates[slot, rs, part * hidden + cs.start:part * hidden + cs.stop] = value
        live = jnp.tile(lens[group, rs, :] > step.astype(F32), (1, COLS // 128))
        return jnp.where(live, out, 0.0).astype(BF16)

    def row_blocks():
        return [slice(r, r + ROWS) for r in range(0, rows, ROWS)]

    def forward_old(group, step):
        def piece(q):
            h = ring_h[group, 1 - lax.rem(step, 2)]
            at = slice(q * hidden, (q + 1) * hidden)
            work[:, at] = mm(h, wrec[q]) + bias_ref[:, at]

        return [functools.partial(piece, q) for q in ORDER]

    def forward_wait(group, step):
        @pl.when(jnp.logical_and(hi, step >= 2))
        def _():
            f_copy(group, step - 2).wait_send()

        @pl.when(lo)
        def _():
            f_copy(group, step).wait_recv()
            fence[...] = jnp.zeros_like(fence)

    def forward_new(group, step, c_ref):
        slot = lax.rem(step, 2)
        x = seq[group, at_step(step), :]
        n_blocks = hidden // COLS
        order = [(q, block) for block in range(n_blocks) for q in (0, 1, 2)] + [(3, block) for block in range(n_blocks)]
        new = {(q, block): mm(x, win[q, :, cols_of(block)]) for q, block in order}
        bent = {}

        def z(q, block, rs):
            return new[q, block][rs] + work[rs, q * hidden + block * COLS:q * hidden + (block + 1) * COLS]

        for block in range(n_blocks):
            cs = cols_of(block)
            for rs in row_blocks():
                in_gate, cand, forget = sigmoid(z(0, block, rs)), jnp.tanh(z(2, block, rs)), sigmoid(z(1, block, rs))
                c_new = forget * c_ref[rs, cs] + in_gate * cand
                c_ref[rs, cs] = c_new
                live = jnp.tile(lens[group, rs, :] > step.astype(F32), (1, COLS // 128))
                bent[block, rs.start] = jnp.where(live, 0.5 * jnp.tanh(c_new), 0.0)
        for block in range(n_blocks):
            for rs in row_blocks():
                out = (jnp.tanh(0.5 * z(3, block, rs)) + 1.0) * bent[block, rs.start]
                ring_h[group, slot, rs, cols_of(block)] = out.astype(BF16)

    def forward_send(group, step):
        @pl.when(hi)
        def _():
            f_copy(group, step).start()

        if group == 0:
            @pl.when(top)
            def _():
                output_error(group, step, lambda rs: ring_h[group, lax.rem(step, 2), rs, :])

    def output_error(group, step, made):
        for rs in row_blocks():
            at = pl.ds(pl.multiple_of(step * rows + rs.start, ROWS), ROWS)
            live = jnp.tile(lens[group, rs, :] > step.astype(F32), (1, hidden // 128))
            error = jnp.where(live, made(rs).astype(F32) - dout[group, at, :].astype(F32), 0.0)
            loss_acc[...] += jnp.sum((error * error).reshape(ROWS // 8, 8, hidden), axis=0)
            dout[group, at, :] = (error * scale).astype(BF16)

    def recompute_mm(group, step):
        x = seq[group, at_step(step), :]
        h = hist[group, at_step(step), :]
        return [{q: mm(x, win[q, :, cols_of(block)]) + mm(h, wrec[q, :, cols_of(block)]) for q in ORDER}
                for block in range(hidden // COLS)]

    def recompute_cell(group, step, slot, c_ref, new, block):
        cs = cols_of(block)
        for rs in row_blocks():
            z = [new[block][q][rs] + bias_of(q, block) for q in range(4)]
            at = pl.ds(pl.multiple_of((step + 1) * rows + rs.start, ROWS), ROWS)
            hist[group, at, cs] = cell(group, step, z, c_ref, rs, cs, slot)

    def backward_wait(group, step):
        @pl.when(jnp.logical_and(lo, step < steps - 2))
        def _():
            b_copy(group, step + 2).wait_send()

        @pl.when(hi)
        def _():
            b_copy(group, step).wait_recv()
            fence[...] = jnp.zeros_like(fence)

        if group == 1:
            @pl.when(jnp.logical_and(top, step >= steps // 2))
            def _():
                for later in (2 * step - steps + 1, 2 * step - steps):
                    output_error(group, later, lambda rs, later=later: hist[
                        group, pl.ds(pl.multiple_of((later + 1) * rows + rs.start, ROWS), ROWS), :])

    def backward_cell(group, step, slot):
        def part(number, rs, cs):
            return gates[slot, rs, number * hidden + cs.start:number * hidden + cs.stop]

        def keep(q, value, rs, cs, sums):
            low = value.astype(BF16)
            now[q, rs, cs] = low
            dz[group][q, pl.ds(pl.multiple_of(step * rows + rs.start, B_ROWS), B_ROWS), cs] = low
            folded = jnp.sum(value.reshape(B_ROWS // 8, 8, COLS), axis=0)
            sums[q] = folded if sums[q] is None else sums[q] + folded

        blocks = [cols_of(block) for block in range(hidden // COLS)]
        pieces = [slice(r, r + B_ROWS) for r in range(0, rows, B_ROWS)]
        for cs in blocks:
            sums = [None] * 4
            for rs in pieces:
                at = pl.ds(pl.multiple_of(step * rows + rs.start, B_ROWS), B_ROWS)
                d_h = dhs[group, rs, cs] + dout[group, at, cs].astype(F32)
                dhs[group, rs, cs] = d_h
                keep(3, d_h * part(3, rs, cs), rs, cs, sums)
            g_bias[3, :, cs] += sums[3]
        for cs in blocks:
            sums = [None] * 4
            for rs in pieces:
                d_cell = dhs[group, rs, cs] * part(4, rs, cs) + dcs[group, rs, cs]
                dcs[group, rs, cs] = d_cell * part(5, rs, cs)
                for q in range(3):
                    keep(q, d_cell * part(q, rs, cs), rs, cs, sums)
            for q in range(3):
                g_bias[q, :, cs] += sums[q]

    def through(weights, store):
        held = [None]
        n_blocks = hidden // COLS

        order = [(block, 3) for block in range(n_blocks)] + [(block, q) for block in range(n_blocks) for q in range(3)]

        def piece(block, q):
            part = mm(now[q, :, cols_of(block)], weights[q, cols_of(block), :])
            held[0] = part if held[0] is None else held[0] + part
            if (block, q) == order[-1]:
                store(held[0])

        return [functools.partial(piece, block, q) for block, q in order]

    def backward_state(group):
        def store(value):
            dhs[group] = value

        return through(wrec_t, store)

    def backward_mm(group, step):
        def store(value):
            ring_d[group, lax.rem(step, 2)] = value.astype(BF16)

        for piece in through(win_t, store):
            piece()

    def backward_send(group, step):
        @pl.when(lo)
        def _():
            b_copy(group, step).start()

    def weight_tile(group, tick):
        q, m = lax.div(tick, 4), lax.rem(tick, 4)
        across = pl.ds(pl.multiple_of(m * (hidden // 4), hidden // 4), hidden // 4)

        def piece(which):
            lhs = seq[group, :, across] if which == 0 else hist[group, 0:steps * rows, across]
            gates[tick, :, which * hidden:(which + 1) * hidden] = mm_t(lhs, dz[group][q])

        return [functools.partial(piece, which) for which in range(2)]

    def tile_copy(tick, which):
        q, m = lax.div(tick, 4), lax.rem(tick, 4)
        part = hidden // 4
        return pltpu.make_async_copy(
            gates.at[tick, :, pl.ds(which * hidden, hidden)],
            partial_ref.at[which, pl.ds(pl.multiple_of(m * part, part), part), pl.ds(pl.multiple_of(q * hidden, hidden), hidden)],
            tile_sem.at[which, tick])

    def phase_1(step, _):
        interleave(forward_old(0, step), [])
        forward_wait(0, step)
        forward_new(0, step, dhs.at[1])
        forward_send(0, step)
        return 0

    @pl.when(jnp.logical_and(lo, hi))
    def _():
        pl.semaphore_wait(barrier, 2)

    @pl.when(jnp.logical_or(first, top))
    def _():
        pl.semaphore_wait(barrier, 1)

    for copy in late_loads:
        copy.start()

    @pl.when(first)
    def _():
        land(inputs_ref, 1).start()

    lax.fori_loop(0, steps, phase_1, 0)
    for copy in late_loads:
        copy.wait()
    first_state(1)

    @pl.when(first)
    def _():
        land(inputs_ref, 1).wait()
        time_major(1, seq)

    again = load(c0_ref.at[pl.ds(rows, rows), :], dhs.at[1], 8)
    again.start()

    def phase_2(step, _):
        new = recompute_mm(0, step)
        recompute_cell(0, step, step, dhs.at[0], new, 0)
        interleave(forward_old(1, step), [])
        recompute_cell(0, step, step, dhs.at[0], new, 1)
        forward_wait(1, step)
        forward_new(1, step, dcs.at[1])
        forward_send(1, step)
        return 0

    lax.fori_loop(0, steps, phase_2, 0)
    again.wait()

    @pl.when(jnp.logical_not(early))
    def _():
        set_up()

    def backward(group, step, slot):
        backward_wait(group, step)
        backward_cell(group, step, slot)
        backward_mm(group, step)
        backward_send(group, step)

    dhs[0] = jnp.zeros((rows, hidden), F32)
    dcs[0] = jnp.zeros((rows, hidden), F32)

    def phase_3(tick, _):
        step = steps - 1 - tick
        backward(0, step, step)
        new = recompute_mm(1, tick)
        recompute_cell(1, tick, steps - tick, dhs.at[1], new, 0)
        interleave(backward_state(0), [])
        recompute_cell(1, tick, steps - tick, dhs.at[1], new, 1)
        return 0

    lax.fori_loop(0, steps, phase_3, 0)
    dhs[1] = jnp.zeros((rows, hidden), F32)
    dcs[1] = jnp.zeros((rows, hidden), F32)

    def tile_copies(tick):
        @pl.when(tick > 0)
        def _():
            for which in range(2):
                tile_copy(tick - 1, which).start()

        @pl.when(tick > 1)
        def _():
            for which in range(2):
                tile_copy(tick - 2, which).wait()

    def loss_on():
        @pl.when(top)
        def _():
            total = jnp.sum(loss_acc[...]) * (0.5 * scale)
            loss_buf[...] = jnp.full(loss_buf.shape, total, F32)

        @pl.when(hi)
        def _():
            loss_copy().wait_recv()

        @pl.when(lo)
        def _():
            loss_copy().start()

    def phase_4(tick, _):
        step = steps - 1 - tick
        backward(1, step, steps - step)

        @pl.when(tick == steps - 4)
        def _():
            loss_on()

        @pl.when(early)
        def _():
            interleave(backward_state(1), [])

        @pl.when(jnp.logical_not(early))
        def _():
            tile_copies(tick)
            interleave(backward_state(1), [])
            interleave(weight_tile(0, tick), [])

        return 0

    lax.fori_loop(0, steps, phase_4, 0)

    def late_tile(tick, _):
        tile_copies(tick)
        interleave(weight_tile(0, tick), [])
        return 0

    @pl.when(early)
    def _():
        lax.fori_loop(0, steps, late_tile, 0)

    for which in range(2):
        last_tile[which] = gates[steps - 1, :, which * hidden:(which + 1) * hidden]
    for which in range(2):
        tile_copy(steps - 2, which).wait()

    @pl.when(hi)
    def _():
        for group in range(2):
            for step in (steps - 2, steps - 1):
                f_copy(group, step).wait_send()

    @pl.when(lo)
    def _():
        for group in range(2):
            for step in (1, 0):
                b_copy(group, step).wait_send()
        loss_copy().wait_send()


def finish_kernel(steps, rows, hidden, partial_ref, dz, hist, seq, dhs, dcs, g_bias, loss_buf, last_tile,
                  loss_ref, g_in_ref, g_rec_ref, g_bias_ref, dh0_ref, dc0_ref, total, in_sem, out_sem, state_sem):
    part = hidden // 4

    def take(q, which, piece):
        cols = pl.ds(pl.multiple_of(q * hidden, hidden), hidden)
        at = pl.ds(0, 3 * part) if piece == 0 else pl.ds(3 * part, part)
        return pltpu.make_async_copy(partial_ref.at[which, at, cols], total.at[q, which, at, :], in_sem.at[q, which, piece])

    def put(q, which):
        cols = pl.ds(pl.multiple_of(q * hidden, hidden), hidden)
        return pltpu.make_async_copy(total.at[q, which], (g_in_ref, g_rec_ref)[which].at[:, cols], out_sem.at[q, which])

    for q in range(4):
        for which in range(2):
            take(q, which, 0).start()
            if q < 3:
                take(q, which, 1).start()
    states = []
    for group in range(2):
        at = pl.ds(group * rows, rows)
        states.append(pltpu.make_async_copy(dhs.at[group], dh0_ref.at[at, :], state_sem.at[group]))
        states.append(pltpu.make_async_copy(dcs.at[group], dc0_ref.at[at, :], state_sem.at[2 + group]))
    for copy in states:
        copy.start()
    loss_ref[0] = loss_buf[0, 0]
    for which in range(2):
        total[3, which, 3 * part:4 * part, :] = last_tile[which]
    for q in range(4):
        g_bias_ref[:, q * hidden:(q + 1) * hidden] = jnp.sum(g_bias[q], axis=0, keepdims=True)

    def gate(q, _):
        new = [mm_t(lhs, dz[q]) for lhs in (seq[1], hist[1, 0:steps * rows, :])]
        for which in range(2):
            take(q, which, 0).wait()

        @pl.when(q < 3)
        def _():
            for which in range(2):
                take(q, which, 1).wait()

        for which in range(2):
            total[q, which] = total[q, which] + new[which]
            put(q, which).start()
        return 0

    lax.fori_loop(0, 4, gate, 0)
    for copy in states:
        copy.wait()
    for q in range(4):
        for which in range(2):
            put(q, which).wait()


def solution(mesh):
    last = mesh.shape['stage'] - 1

    def local(inputs, targets, lengths, w_in, w_rec, bias, h_init, c_init):
        batch, steps, hidden = inputs.shape
        rows = batch // 2
        wide = 4 * hidden
        any_spec = pl.BlockSpec(memory_space=pl.ANY)
        vmem_spec = pl.BlockSpec(memory_space=pltpu.VMEM)
        dma = pltpu.SemaphoreType.DMA
        held = pl.pallas_call(
            functools.partial(kernel, last, steps, rows, hidden),
            out_shape=(
                jax.ShapeDtypeStruct((8, hidden, wide), F32),
                pltpu.VMEM((4, steps * rows, hidden), BF16),
                pltpu.VMEM((2, (steps + 1) * rows, hidden), BF16),
                pltpu.VMEM((2, steps * rows, hidden), BF16),
                pltpu.VMEM((2, rows, hidden), F32),
                pltpu.VMEM((2, rows, hidden), F32),
                pltpu.VMEM((4, 8, hidden), F32),
                pltpu.VMEM((8, 128), F32),
                pltpu.VMEM((2, hidden // 4, hidden), F32)),
            in_specs=[any_spec] * 8,
            out_specs=(any_spec,) + (vmem_spec,) * 8,
            scratch_shapes=[
                pltpu.VMEM((steps + 1, rows, 6 * hidden), F32),
                pltpu.VMEM((4, steps * rows, hidden), BF16),
                pltpu.VMEM((4, rows, hidden), BF16),
                pltpu.VMEM((2, steps * rows, hidden), BF16),
                pltpu.VMEM((4, hidden, hidden), BF16),
                pltpu.VMEM((4, hidden, hidden), BF16),
                pltpu.VMEM((2, 2, rows, hidden), BF16),
                pltpu.VMEM((2, 2, rows, hidden), BF16),
                pltpu.VMEM((rows, 4 * hidden), F32),
                pltpu.VMEM((2, rows, 128), F32),
                pltpu.VMEM((8, hidden), F32),
                pltpu.VMEM((32, 128), F32),
                pltpu.VMEM((8, wide), F32),
                pltpu.VMEM((32, 128), jnp.int32),
                dma((2, steps)), dma((2, 2)), dma((2, steps)), dma((2, 2)), dma, dma, dma((17,)), dma((2, steps))],
            compiler_params=pltpu.CompilerParams(
                collective_id=0, has_side_effects=True, vmem_limit_bytes=HELD_LIMIT),
        )(inputs.reshape(batch * steps, hidden), targets.reshape(batch * steps, hidden), lengths.reshape(2, rows),
          w_in[0], w_rec[0], bias, h_init[0], c_init[0])
        loss, g_in, g_rec, g_bias, dh0, dc0 = pl.pallas_call(
            functools.partial(finish_kernel, steps, rows, hidden),
            out_shape=(
                jax.ShapeDtypeStruct((1,), F32),
                jax.ShapeDtypeStruct((hidden, wide), F32),
                jax.ShapeDtypeStruct((hidden, wide), F32),
                jax.ShapeDtypeStruct((1, wide), F32),
                jax.ShapeDtypeStruct((batch, hidden), F32),
                jax.ShapeDtypeStruct((batch, hidden), F32)),
            in_specs=[pl.BlockSpec(memory_space=pltpu.HBM)] + [vmem_spec] * 8,
            out_specs=(pl.BlockSpec(memory_space=pltpu.SMEM), any_spec, any_spec, vmem_spec, any_spec, any_spec),
            scratch_shapes=[pltpu.VMEM((4, 2, hidden, hidden), F32), dma((4, 2, 2)), dma((4, 2)), dma((4,))],
            compiler_params=pltpu.CompilerParams(vmem_limit_bytes=FINISH_LIMIT),
        )(*held)
        return loss, g_in[None], g_rec[None], g_bias, dh0[None], dc0[None]

    layer_spec = P(('data', 'stage'))
    return jax.shard_map(
        local, mesh=mesh,
        in_specs=(P('data'), P('data'), P('data'), P('stage'), P('stage'), P('stage'), P('stage', 'data'), P('stage', 'data')),
        out_specs=(P('data'), layer_spec, layer_spec, layer_spec, P('stage', 'data'), P('stage', 'data')),
        check_vma=False)
```

```python
import functools

import jax
import jax.numpy as jnp
from jax import lax
from jax.experimental import pallas as pl
from jax.experimental.pallas import tpu as pltpu
from jax.sharding import PartitionSpec as P

F32 = jnp.float32
BF16 = jnp.bfloat16
COLS = 256
ROWS = 32
B_ROWS = 16
ORDER = (0, 2, 1, 3)
HELD_LIMIT = 48_200_000
FINISH_LIMIT = 16_000_000


def mm(lhs, rhs):
    return jnp.dot(lhs, rhs, preferred_element_type=F32)


def mm_t(lhs, rhs):
    return lax.dot_general(lhs, rhs, (((0,), (0,)), ((), ())), preferred_element_type=F32)


def sigmoid(value):
    return 0.5 * jnp.tanh(0.5 * value) + 0.5


def interleave(main, side):
    done = 0
    for idx, piece in enumerate(main):
        upto = (idx + 1) * len(side) // len(main)
        for other in side[done:upto]:
            other()
        done = upto
        piece()


def kernel(last, steps, rows, hidden,
           inputs_ref, targets_ref, lens_hbm, w_in_ref, w_rec_ref, bias_hbm, h0_ref, c0_ref,
           partial_ref, dz_1, hist, seq, dhs, dcs, g_bias, loss_buf, last_tile,
           gates, dz_0, now, dout, win_t, wrec_t, ring_h, ring_d, work, lens, loss_acc, fence, bias_all, lens_all,
           f_recv, f_send, b_recv, b_send, loss_recv, loss_send, local_sem, tile_sem):
    stage = lax.axis_index('stage')
    bias_ref = bias_all.at[pl.ds(0, 1)]
    lens_ref = lens_all.at[pl.ds(0, 2)]
    lo, hi = stage > 0, stage < last
    first, top = stage == 0, stage == last
    dz = (dz_0, dz_1)
    win, wrec = dz_1.at[:, pl.ds(0, hidden), :], dz_1.at[:, pl.ds(hidden, hidden), :]
    batch = 2 * rows
    scale = 1.0 / (batch * steps)

    def at_step(step):
        return pl.ds(pl.multiple_of(step * rows, rows), rows)

    def f_copy(group, step):
        slot = lax.rem(step, 2)
        return pltpu.make_async_remote_copy(
            src_ref=ring_h.at[group, slot], dst_ref=seq.at[group, at_step(step), :],
            send_sem=f_send.at[group, slot], recv_sem=f_recv.at[group, step],
            device_id={'stage': stage + 1}, device_id_type=pl.DeviceIdType.MESH)

    def b_copy(group, step):
        slot = lax.rem(step, 2)
        return pltpu.make_async_remote_copy(
            src_ref=ring_d.at[group, slot], dst_ref=dout.at[group, at_step(step), :],
            send_sem=b_send.at[group, slot], recv_sem=b_recv.at[group, step],
            device_id={'stage': stage - 1}, device_id_type=pl.DeviceIdType.MESH)

    def loss_copy():
        return pltpu.make_async_remote_copy(
            src_ref=loss_buf, dst_ref=loss_buf, send_sem=loss_send, recv_sem=loss_recv,
            device_id={'stage': stage - 1}, device_id_type=pl.DeviceIdType.MESH)

    def load(src, dst, sem):
        return pltpu.make_async_copy(src, dst, local_sem.at[sem])

    smalls = [load(lens_hbm, lens_ref, 15), load(bias_hbm, bias_ref, 16)]
    for copy in smalls:
        copy.start()
    loads = []
    for q in range(4):
        cols = pl.ds(q * hidden, hidden)
        loads.append(load(w_rec_ref.at[:, cols], wrec.at[q], 4 + q))
    for q in range(4):
        cols = pl.ds(q * hidden, hidden)
        loads.append(load(w_in_ref.at[:, cols], win.at[q], 0 + q))
    loads.append(load(c0_ref.at[pl.ds(0, rows), :], dhs.at[1], 8))
    loads.append(load(h0_ref.at[pl.ds(0, rows), :], gates.at[0, :, pl.ds(0, hidden)], 11))
    late_loads = [
        load(c0_ref.at[pl.ds(rows, rows), :], dcs.at[1], 9),
        load(c0_ref.at[pl.ds(0, rows), :], dhs.at[0], 10),
        load(h0_ref.at[pl.ds(rows, rows), :], gates.at[1, :, pl.ds(0, hidden)], 12)]

    def land(src, group):
        return load(src.at[pl.ds(group * rows * steps, rows * steps), :],
                    dz_0.at[group], 13 + group)

    @pl.when(first)
    def _():
        land(inputs_ref, 0).start()

    for copy in loads[8:] + loads[:8]:
        copy.start()

    @pl.when(top)
    def _():
        for group in range(2):
            land(targets_ref, group).start()

    barrier = pltpu.get_barrier_semaphore()

    @pl.when(lo)
    def _():
        pl.semaphore_signal(barrier, inc=1, device_id={'stage': stage - 1}, device_id_type=pl.DeviceIdType.MESH)

    @pl.when(hi)
    def _():
        pl.semaphore_signal(barrier, inc=1, device_id={'stage': stage + 1}, device_id_type=pl.DeviceIdType.MESH)

    for copy in smalls:
        copy.wait()
    for group in range(2):
        row = lens_ref[group:group + 1, :].astype(F32)
        lens[group] = jnp.broadcast_to(row, (128, rows)).T

    loss_acc[...] = jnp.zeros_like(loss_acc)
    g_bias[...] = jnp.zeros_like(g_bias)
    dcs[0] = jnp.zeros((rows, hidden), F32)

    def time_major(group, dst):
        size = 16 * steps
        out_row = lax.broadcasted_iota(jnp.int32, (size, size), 0)
        in_row = lax.broadcasted_iota(jnp.int32, (size, size), 1)
        step_of, row_of = lax.div(out_row, 16), lax.rem(out_row, 16)
        permute = (in_row == row_of * steps + step_of).astype(F32).astype(BF16)

        def blocks(trip, _):
            for idx in [trip * 4 + sub for sub in range(4)]:
                piece = dz_0[group, pl.ds(pl.multiple_of(idx * size, size), size), :]
                moved = mm(permute, piece).astype(BF16)
                for step in range(steps):
                    dst[group, pl.ds(pl.multiple_of(step * rows + idx * 16, 16), 16), :] = moved[step * 16:(step + 1) * 16]
            return 0

        lax.fori_loop(0, rows // 64, blocks, 0)

    def set_up():
        def turn(q, _):
            win_t[q] = win[q].T
            wrec_t[q] = wrec[q].T
            return 0

        lax.fori_loop(0, 4, turn, 0)

    @pl.when(first)
    def _():
        land(inputs_ref, 0).wait()
        time_major(0, seq)

    for copy in loads[8:]:
        copy.wait()

    def first_state(group):
        h_start = gates[group, :, 0:hidden].astype(BF16)
        hist[group, 0:rows, :] = h_start
        ring_h[group, 1] = h_start

    first_state(0)

    @pl.when(top)
    def _():
        for group in range(2):
            land(targets_ref, group).wait()
            time_major(group, dout)

    for copy in loads[:8]:
        copy.wait()
    early = stage >= (last + 1) // 2

    @pl.when(early)
    def _():
        set_up()

    def cols_of(block):
        return slice(block * COLS, (block + 1) * COLS)

    def bias_of(q, block):
        return bias_ref[:, q * hidden + block * COLS:q * hidden + (block + 1) * COLS]

    def cell(group, step, z, c_ref, rs, cs, slot=None):
        in_gate, cand = sigmoid(z[0]), jnp.tanh(z[2])
        forget = sigmoid(z[1])
        new, old = in_gate * cand, forget * c_ref[rs, cs]
        c_new = old + new
        c_ref[rs, cs] = c_new
        tanh_c = jnp.tanh(c_new)
        out_gate = sigmoid(z[3])
        out = out_gate * tanh_c
        if slot is not None:
            values = (new * (1.0 - in_gate), old * (1.0 - forget), in_gate - new * cand, out * (1.0 - out_gate),
                      out_gate - out * tanh_c, forget)
            for part, value in enumerate(values):
                gates[slot, rs, part * hidden + cs.start:part * hidden + cs.stop] = value
        live = jnp.tile(lens[group, rs, :] > step.astype(F32), (1, COLS // 128))
        return jnp.where(live, out, 0.0).astype(BF16)

    def row_blocks():
        return [slice(r, r + ROWS) for r in range(0, rows, ROWS)]

    def forward_old(group, step):
        def piece(q):
            h = ring_h[group, 1 - lax.rem(step, 2)]
            at = slice(q * hidden, (q + 1) * hidden)
            work[:, at] = mm(h, wrec[q]) + bias_ref[:, at]

        return [functools.partial(piece, q) for q in ORDER]

    def forward_wait(group, step):
        @pl.when(jnp.logical_and(hi, step >= 2))
        def _():
            f_copy(group, step - 2).wait_send()

        @pl.when(lo)
        def _():
            f_copy(group, step).wait_recv()
            fence[...] = jnp.zeros_like(fence)

    def forward_new(group, step, c_ref):
        slot = lax.rem(step, 2)
        x = seq[group, at_step(step), :]
        n_blocks = hidden // COLS
        order = [(q, block) for block in range(n_blocks) for q in (0, 1, 2)] + [(3, block) for block in range(n_blocks)]
        new = {(q, block): mm(x, win[q, :, cols_of(block)]) for q, block in order}
        bent = {}

        def z(q, block, rs):
            return new[q, block][rs] + work[rs, q * hidden + block * COLS:q * hidden + (block + 1) * COLS]

        for block in range(n_blocks):
            cs = cols_of(block)
            for rs in row_blocks():
                in_gate, cand, forget = sigmoid(z(0, block, rs)), jnp.tanh(z(2, block, rs)), sigmoid(z(1, block, rs))
                c_new = forget * c_ref[rs, cs] + in_gate * cand
                c_ref[rs, cs] = c_new
                live = jnp.tile(lens[group, rs, :] > step.astype(F32), (1, COLS // 128))
                bent[block, rs.start] = jnp.where(live, 0.5 * jnp.tanh(c_new), 0.0)
        for block in range(n_blocks):
            for rs in row_blocks():
                out = (jnp.tanh(0.5 * z(3, block, rs)) + 1.0) * bent[block, rs.start]
                ring_h[group, slot, rs, cols_of(block)] = out.astype(BF16)

    def forward_send(group, step):
        @pl.when(hi)
        def _():
            f_copy(group, step).start()

        if group == 0:
            @pl.when(top)
            def _():
                output_error(group, step, lambda rs: ring_h[group, lax.rem(step, 2), rs, :])

    def output_error(group, step, made):
        for rs in row_blocks():
            at = pl.ds(pl.multiple_of(step * rows + rs.start, ROWS), ROWS)
            live = jnp.tile(lens[group, rs, :] > step.astype(F32), (1, hidden // 128))
            error = jnp.where(live, made(rs).astype(F32) - dout[group, at, :].astype(F32), 0.0)
            loss_acc[...] += jnp.sum((error * error).reshape(ROWS // 8, 8, hidden), axis=0)
            dout[group, at, :] = (error * scale).astype(BF16)

    def recompute_mm(group, step):
        x = seq[group, at_step(step), :]
        h = hist[group, at_step(step), :]
        return [{q: mm(x, win[q, :, cols_of(block)]) + mm(h, wrec[q, :, cols_of(block)]) for q in ORDER}
                for block in range(hidden // COLS)]

    def recompute_cell(group, step, slot, c_ref, new, block):
        cs = cols_of(block)
        for rs in row_blocks():
            z = [new[block][q][rs] + bias_of(q, block) for q in range(4)]
            at = pl.ds(pl.multiple_of((step + 1) * rows + rs.start, ROWS), ROWS)
            hist[group, at, cs] = cell(group, step, z, c_ref, rs, cs, slot)

    def backward_wait(group, step):
        @pl.when(jnp.logical_and(lo, step < steps - 2))
        def _():
            b_copy(group, step + 2).wait_send()

        @pl.when(hi)
        def _():
            b_copy(group, step).wait_recv()
            fence[...] = jnp.zeros_like(fence)

        if group == 1:
            @pl.when(jnp.logical_and(top, step >= steps // 2))
            def _():
                for later in (2 * step - steps + 1, 2 * step - steps):
                    output_error(group, later, lambda rs, later=later: hist[
                        group, pl.ds(pl.multiple_of((later + 1) * rows + rs.start, ROWS), ROWS), :])

    def backward_cell(group, step, slot):
        def part(number, rs, cs):
            return gates[slot, rs, number * hidden + cs.start:number * hidden + cs.stop]

        def keep(q, value, rs, cs, sums):
            low = value.astype(BF16)
            now[q, rs, cs] = low
            dz[group][q, pl.ds(pl.multiple_of(step * rows + rs.start, B_ROWS), B_ROWS), cs] = low
            folded = jnp.sum(value.reshape(B_ROWS // 8, 8, COLS), axis=0)
            sums[q] = folded if sums[q] is None else sums[q] + folded

        blocks = [cols_of(block) for block in range(hidden // COLS)]
        pieces = [slice(r, r + B_ROWS) for r in range(0, rows, B_ROWS)]
        for cs in blocks:
            sums = [None] * 4
            for rs in pieces:
                at = pl.ds(pl.multiple_of(step * rows + rs.start, B_ROWS), B_ROWS)
                d_h = dhs[group, rs, cs] + dout[group, at, cs].astype(F32)
                dhs[group, rs, cs] = d_h
                keep(3, d_h * part(3, rs, cs), rs, cs, sums)
            g_bias[3, :, cs] += sums[3]
        for cs in blocks:
            sums = [None] * 4
            for rs in pieces:
                d_cell = dhs[group, rs, cs] * part(4, rs, cs) + dcs[group, rs, cs]
                dcs[group, rs, cs] = d_cell * part(5, rs, cs)
                for q in range(3):
                    keep(q, d_cell * part(q, rs, cs), rs, cs, sums)
            for q in range(3):
                g_bias[q, :, cs] += sums[q]

    def through(weights, store):
        held = [None]
        n_blocks = hidden // COLS

        order = [(block, 3) for block in range(n_blocks)] + [(block, q) for block in range(n_blocks) for q in range(3)]

        def piece(block, q):
            part = mm(now[q, :, cols_of(block)], weights[q, cols_of(block), :])
            held[0] = part if held[0] is None else held[0] + part
            if (block, q) == order[-1]:
                store(held[0])

        return [functools.partial(piece, block, q) for block, q in order]

    def backward_state(group):
        def store(value):
            dhs[group] = value

        return through(wrec_t, store)

    def backward_mm(group, step):
        def store(value):
            ring_d[group, lax.rem(step, 2)] = value.astype(BF16)

        for piece in through(win_t, store):
            piece()

    def backward_send(group, step):
        @pl.when(lo)
        def _():
            b_copy(group, step).start()

    def weight_tile(group, tick):
        q, m = lax.div(tick, 4), lax.rem(tick, 4)
        across = pl.ds(pl.multiple_of(m * (hidden // 4), hidden // 4), hidden // 4)

        def piece(which):
            lhs = seq[group, :, across] if which == 0 else hist[group, 0:steps * rows, across]
            gates[tick, :, which * hidden:(which + 1) * hidden] = mm_t(lhs, dz[group][q])

        return [functools.partial(piece, which) for which in range(2)]

    def tile_copy(tick, which):
        q, m = lax.div(tick, 4), lax.rem(tick, 4)
        part = hidden // 4
        return pltpu.make_async_copy(
            gates.at[tick, :, pl.ds(which * hidden, hidden)],
            partial_ref.at[which, pl.ds(pl.multiple_of(m * part, part), part), pl.ds(pl.multiple_of(q * hidden, hidden), hidden)],
            tile_sem.at[which, tick])

    def phase_1(step, _):
        interleave(forward_old(0, step), [])
        forward_wait(0, step)
        forward_new(0, step, dhs.at[1])
        forward_send(0, step)
        return 0

    @pl.when(jnp.logical_and(lo, hi))
    def _():
        pl.semaphore_wait(barrier, 2)

    @pl.when(jnp.logical_or(first, top))
    def _():
        pl.semaphore_wait(barrier, 1)

    for copy in late_loads:
        copy.start()

    @pl.when(first)
    def _():
        land(inputs_ref, 1).start()

    lax.fori_loop(0, steps, phase_1, 0)
    for copy in late_loads:
        copy.wait()
    first_state(1)

    @pl.when(first)
    def _():
        land(inputs_ref, 1).wait()
        time_major(1, seq)

    again = load(c0_ref.at[pl.ds(rows, rows), :], dhs.at[1], 8)
    again.start()

    def phase_2(step, _):
        new = recompute_mm(0, step)
        recompute_cell(0, step, step, dhs.at[0], new, 0)
        interleave(forward_old(1, step), [])
        recompute_cell(0, step, step, dhs.at[0], new, 1)
        forward_wait(1, step)
        forward_new(1, step, dcs.at[1])
        forward_send(1, step)
        return 0

    lax.fori_loop(0, steps, phase_2, 0)
    again.wait()

    @pl.when(jnp.logical_not(early))
    def _():
        set_up()

    def backward(group, step, slot):
        backward_wait(group, step)
        backward_cell(group, step, slot)
        backward_mm(group, step)
        backward_send(group, step)

    dhs[0] = jnp.zeros((rows, hidden), F32)

    def phase_3(tick, _):
        step = steps - 1 - tick
        backward(0, step, step)
        new = recompute_mm(1, tick)
        recompute_cell(1, tick, steps - tick, dhs.at[1], new, 0)
        interleave(backward_state(0), [])
        recompute_cell(1, tick, steps - tick, dhs.at[1], new, 1)
        return 0

    lax.fori_loop(0, steps, phase_3, 0)
    dhs[1] = jnp.zeros((rows, hidden), F32)
    dcs[1] = jnp.zeros((rows, hidden), F32)

    def tile_copies(tick):
        @pl.when(tick > 0)
        def _():
            for which in range(2):
                tile_copy(tick - 1, which).start()

        @pl.when(tick > 1)
        def _():
            for which in range(2):
                tile_copy(tick - 2, which).wait()

    def loss_on():
        @pl.when(top)
        def _():
            total = jnp.sum(loss_acc[...]) * (0.5 * scale)
            loss_buf[...] = jnp.full(loss_buf.shape, total, F32)

        @pl.when(hi)
        def _():
            loss_copy().wait_recv()

        @pl.when(lo)
        def _():
            loss_copy().start()

    def phase_4(tick, _):
        step = steps - 1 - tick
        backward(1, step, steps - step)

        @pl.when(tick == steps - 4)
        def _():
            loss_on()

        @pl.when(early)
        def _():
            interleave(backward_state(1), [])

        @pl.when(jnp.logical_not(early))
        def _():
            tile_copies(tick)
            interleave(backward_state(1), [])
            interleave(weight_tile(0, tick), [])

        return 0

    lax.fori_loop(0, steps, phase_4, 0)

    def late_tile(tick, _):
        tile_copies(tick)
        interleave(weight_tile(0, tick), [])
        return 0

    @pl.when(early)
    def _():
        lax.fori_loop(0, steps, late_tile, 0)

    for which in range(2):
        last_tile[which] = gates[steps - 1, :, which * hidden:(which + 1) * hidden]
    for which in range(2):
        tile_copy(steps - 2, which).wait()

    @pl.when(hi)
    def _():
        for group in range(2):
            for step in (steps - 2, steps - 1):
                f_copy(group, step).wait_send()

    @pl.when(lo)
    def _():
        for group in range(2):
            for step in (1, 0):
                b_copy(group, step).wait_send()
        loss_copy().wait_send()


def finish_kernel(steps, rows, hidden, partial_ref, dz, hist, seq, dhs, dcs, g_bias, loss_buf, last_tile,
                  loss_ref, g_in_ref, g_rec_ref, g_bias_ref, dh0_ref, dc0_ref, total, in_sem, out_sem, state_sem):
    part = hidden // 4

    def take(q, which, piece):
        cols = pl.ds(pl.multiple_of(q * hidden, hidden), hidden)
        at = pl.ds(0, 3 * part) if piece == 0 else pl.ds(3 * part, part)
        return pltpu.make_async_copy(partial_ref.at[which, at, cols], total.at[q, which, at, :], in_sem.at[q, which, piece])

    def put(q, which):
        cols = pl.ds(pl.multiple_of(q * hidden, hidden), hidden)
        return pltpu.make_async_copy(total.at[q, which], (g_in_ref, g_rec_ref)[which].at[:, cols], out_sem.at[q, which])

    for q in range(4):
        for which in range(2):
            take(q, which, 0).start()
            if q < 3:
                take(q, which, 1).start()
    states = []
    for group in range(2):
        at = pl.ds(group * rows, rows)
        states.append(pltpu.make_async_copy(dhs.at[group], dh0_ref.at[at, :], state_sem.at[group]))
        states.append(pltpu.make_async_copy(dcs.at[group], dc0_ref.at[at, :], state_sem.at[2 + group]))
    for copy in states:
        copy.start()
    loss_ref[0] = loss_buf[0, 0]
    for which in range(2):
        total[3, which, 3 * part:4 * part, :] = last_tile[which]
    for q in range(4):
        g_bias_ref[:, q * hidden:(q + 1) * hidden] = jnp.sum(g_bias[q], axis=0, keepdims=True)

    def gate(q, _):
        new = [mm_t(lhs, dz[q]) for lhs in (seq[1], hist[1, 0:steps * rows, :])]
        for which in range(2):
            take(q, which, 0).wait()

        @pl.when(q < 3)
        def _():
            for which in range(2):
                take(q, which, 1).wait()

        for which in range(2):
            total[q, which] = total[q, which] + new[which]
            put(q, which).start()
        return 0

    lax.fori_loop(0, 4, gate, 0)
    for copy in states:
        copy.wait()
    for q in range(4):
        for which in range(2):
            put(q, which).wait()


def solution(mesh):
    last = mesh.shape['stage'] - 1

    def local(inputs, targets, lengths, w_in, w_rec, bias, h_init, c_init):
        batch, steps, hidden = inputs.shape
        rows = batch // 2
        wide = 4 * hidden
        any_spec = pl.BlockSpec(memory_space=pl.ANY)
        vmem_spec = pl.BlockSpec(memory_space=pltpu.VMEM)
        dma = pltpu.SemaphoreType.DMA
        held = pl.pallas_call(
            functools.partial(kernel, last, steps, rows, hidden),
            out_shape=(
                jax.ShapeDtypeStruct((8, hidden, wide), F32),
                pltpu.VMEM((4, steps * rows, hidden), BF16),
                pltpu.VMEM((2, (steps + 1) * rows, hidden), BF16),
                pltpu.VMEM((2, steps * rows, hidden), BF16),
                pltpu.VMEM((2, rows, hidden), F32),
                pltpu.VMEM((2, rows, hidden), F32),
                pltpu.VMEM((4, 8, hidden), F32),
                pltpu.VMEM((8, 128), F32),
                pltpu.VMEM((2, hidden // 4, hidden), F32)),
            in_specs=[any_spec] * 8,
            out_specs=(any_spec,) + (vmem_spec,) * 8,
            scratch_shapes=[
                pltpu.VMEM((steps + 1, rows, 6 * hidden), F32),
                pltpu.VMEM((4, steps * rows, hidden), BF16),
                pltpu.VMEM((4, rows, hidden), BF16),
                pltpu.VMEM((2, steps * rows, hidden), BF16),
                pltpu.VMEM((4, hidden, hidden), BF16),
                pltpu.VMEM((4, hidden, hidden), BF16),
                pltpu.VMEM((2, 2, rows, hidden), BF16),
                pltpu.VMEM((2, 2, rows, hidden), BF16),
                pltpu.VMEM((rows, 4 * hidden), F32),
                pltpu.VMEM((2, rows, 128), F32),
                pltpu.VMEM((8, hidden), F32),
                pltpu.VMEM((32, 128), F32),
                pltpu.VMEM((8, wide), F32),
                pltpu.VMEM((32, 128), jnp.int32),
                dma((2, steps)), dma((2, 2)), dma((2, steps)), dma((2, 2)), dma, dma, dma((17,)), dma((2, steps))],
            compiler_params=pltpu.CompilerParams(
                collective_id=0, has_side_effects=True, vmem_limit_bytes=HELD_LIMIT),
        )(inputs.reshape(batch * steps, hidden), targets.reshape(batch * steps, hidden), lengths.reshape(2, rows),
          w_in[0], w_rec[0], bias, h_init[0], c_init[0])
        loss, g_in, g_rec, g_bias, dh0, dc0 = pl.pallas_call(
            functools.partial(finish_kernel, steps, rows, hidden),
            out_shape=(
                jax.ShapeDtypeStruct((1,), F32),
                jax.ShapeDtypeStruct((hidden, wide), F32),
                jax.ShapeDtypeStruct((hidden, wide), F32),
                jax.ShapeDtypeStruct((1, wide), F32),
                jax.ShapeDtypeStruct((batch, hidden), F32),
                jax.ShapeDtypeStruct((batch, hidden), F32)),
            in_specs=[pl.BlockSpec(memory_space=pltpu.HBM)] + [vmem_spec] * 8,
            out_specs=(pl.BlockSpec(memory_space=pltpu.SMEM), any_spec, any_spec, vmem_spec, any_spec, any_spec),
            scratch_shapes=[pltpu.VMEM((4, 2, hidden, hidden), F32), dma((4, 2, 2)), dma((4, 2)), dma((4,))],
            compiler_params=pltpu.CompilerParams(vmem_limit_bytes=FINISH_LIMIT),
        )(*held)
        return loss, g_in[None], g_rec[None], g_bias, dh0[None], dc0[None]

    layer_spec = P(('data', 'stage'))
    return jax.shard_map(
        local, mesh=mesh,
        in_specs=(P('data'), P('data'), P('data'), P('stage'), P('stage'), P('stage'), P('stage', 'data'), P('stage', 'data')),
        out_specs=(P('data'), layer_spec, layer_spec, layer_spec, P('stage', 'data'), P('stage', 'data')),
        check_vma=False)
```
